32 devices in a mesh: ccy: 4 (over x, core), path: 8 (over z, y).
Axes of the slice: x: 2, y: 2, z: 4, core: 2. Of those that a mesh axis runs over, the one named last changes fastest.
Arguments:
- curve_store: bfloat16 [4, 16, 64, 2048], P('ccy', 'path'), may hold values from -0.13 to 0.18
- cash_index: int32 [4, 2048, 16], P('ccy'), may hold values from 0 to 1023
- cash_amount: float32 [4, 2048, 16], P('ccy'), may hold values from -0.6 to 0.6
- trade_set: int32 [4, 2048], P('ccy'), may hold values from 0 to 511
- date_slot: int32 [16], replicated, may hold values from 0 to 15, as said below
- default_weight: float32 [16, 512], replicated, may hold values from 0.02 to 0.2
Outputs:
- exposure: float32 [16, 512], P(None, 'ccy')
- node_sens: float32 [4, 16, 64], P('ccy')
The draws below stay inside these ranges and needn't reach their ends.
Inputs may be any that keep to these rules, and one draw needn't show every extreme that they name: `date_slot`: the 16 slots are distinct; slot s is stored at path index s // 2, position s % 2.
All inputs are finite; a program needn't handle non-finite values.
Results may differ from the reference program's by a relative error of at most 0.0029.
Values may be sent and summed in bfloat16 or wider, within the bound.
No kernel may reach another device: no remote copies, remote signals or barrier semaphores. Data moves between devices by JAX's collectives and lax.ppermute only.
A program may use at most 64 MiB of HBM per device.

```python
import math
import jax
import jax.numpy as jnp
from jax import lax

NODES = 64
CFG = 1024
NSETS = 512
TRADES = 2048
NCF = 16
DATES = 16
PATHS = 2048
SLOTS_ALL = 16
N_CCY = 4


def draw_date_slot(key, part):
    return jax.random.permutation(key, SLOTS_ALL)[:DATES].astype(jnp.int32)


def draw_curve_store(key, part):
    level_key, spread_key, height_key, flip_key = jax.random.split(jax.random.fold_in(key, 7), 4)
    block_shape = (N_CCY, SLOTS_ALL, 1, PATHS)
    base_level = jax.random.uniform(level_key, block_shape, jnp.float32, 0.0, 0.05)
    jump_scale = jnp.exp(jax.random.uniform(spread_key, block_shape, jnp.float32, math.log(0.01), math.log(0.12)))
    jump_height = jax.random.uniform(height_key, (N_CCY, SLOTS_ALL, NODES, PATHS), jnp.float32, 0.5, 1.0)
    flip_bits = jax.random.randint(flip_key, block_shape, 0, 2)
    node_index = jnp.arange(NODES, dtype=jnp.int32).reshape(1, 1, NODES, 1)
    parity = (node_index + flip_bits) % 2
    signed = 1.0 - 2.0 * parity.astype(jnp.float32)
    return (base_level + jump_scale * signed * jump_height).astype(jnp.bfloat16)


def touch_ends(drawn, key, least, largest):
    spot = [jax.random.randint(jax.random.fold_in(key, axis), (), 0, length) for axis, length in enumerate(drawn.shape)]
    main_axis = drawn.shape.index(max(drawn.shape))
    neighbour = spot[:main_axis] + [(spot[main_axis] + 1) % drawn.shape[main_axis]] + spot[main_axis + 1:]
    return drawn.at[tuple(spot)].set(least).at[tuple(neighbour)].set(largest)


def level_of(own_key, dims, shards, least, top_value):
    def one(dim, blocks):
        draws = jax.random.uniform(jax.random.fold_in(jax.random.fold_in(own_key, 6), dim), (blocks,), jnp.float32, least / len(shards), top_value / len(shards))
        return jnp.repeat(jnp.exp(draws), dims[dim] // blocks).reshape((-1,) + (1,) * (len(dims) - dim - 1))

    gain = one(*shards[0])
    for cut in shards[1:]:
        gain = gain * one(*cut)
    return gain


def noise(stream_key, extent, scale, most, shards=(), held_as=jnp.bfloat16):
    entries = jax.random.normal(stream_key, extent, jnp.float32) * scale
    if len(shards) > 0:
        entries = level_of(stream_key, extent, shards, -0.22, 0.18) * entries
    return jnp.clip(entries, min=-most, max=most).astype(held_as)


def setup_inputs(seed: int = 0) -> dict:
    key_list = jax.random.split(jax.random.key(seed), 7)
    return {
        "curve_store": draw_curve_store(jax.random.fold_in(key_list[6], 71), 0),
        "cash_index": touch_ends(jax.random.randint(key_list[1], (N_CCY, TRADES, NCF), 0, CFG), jax.random.fold_in(key_list[1], 1), 0, CFG - 1).astype(jnp.int32),
        "cash_amount": noise(key_list[2], (N_CCY, TRADES, NCF), 0.1, 0.6, ((0, 4),), jnp.float32),
        "trade_set": touch_ends(jax.random.randint(key_list[3], (N_CCY, TRADES), 0, NSETS), jax.random.fold_in(key_list[3], 1), 0, NSETS - 1).astype(jnp.int32),
        "date_slot": draw_date_slot(jax.random.fold_in(key_list[6], 71), 0),
        "default_weight": jnp.clip(jnp.exp(jax.random.uniform(key_list[5], (DATES, NSETS), jnp.float32, math.log(0.02), math.log(0.2))), 0.02, 0.2),
    }


SOFTEN = 0.04
HORIZON = 32.0

def date_tables(date_index, node_count, grid_count):
    start_time = 0.5 * (jnp.asarray(date_index).astype(jnp.float32) + 1.0)
    grid_times = HORIZON * (jnp.arange(grid_count, dtype=jnp.float32) + 1.0) / grid_count
    tenors = HORIZON * (jnp.arange(node_count, dtype=jnp.float32) + 1.0) / node_count
    remain = grid_times - start_time
    alive_mask = (remain > 0.0).astype(jnp.float32)
    clipped = jnp.clip(remain, HORIZON / node_count, HORIZON)
    weights = jnp.maximum(0.0, 1.0 - jnp.abs(clipped[None, :] - tenors[:, None]) * (node_count / HORIZON))
    return (remain, alive_mask, weights)

def netted_cash(flow_index, amount, trade_sets):
    columns = jnp.repeat(trade_sets, flow_index.shape[1]).astype(jnp.int32)
    cash_table = jnp.zeros((CFG, NSETS), jnp.float32).at[flow_index.reshape(-1).astype(jnp.int32), columns].add(amount.reshape(-1).astype(jnp.float32))
    return cash_table.astype(jnp.bfloat16)

def reference(curve_store, cash_index, cash_amount, trade_set, date_slot, default_weight):
    total_paths = curve_store.shape[3]
    tables = [netted_cash(cash_index[member], cash_amount[member], trade_set[member]) for member in range(N_CCY)]
    exposure_rows = []
    sens_rows = []
    for date_index in range(DATES):
        remain, alive_mask, weights = date_tables(date_index, NODES, CFG)
        grid_weights = weights.astype(jnp.bfloat16)
        values = jnp.zeros((total_paths, NSETS), jnp.float32)
        discounts = []
        for member in range(N_CCY):
            curve_now = lax.dynamic_index_in_dim(curve_store[member], date_slot[date_index].astype(jnp.int32), 0, keepdims=False)
            yields = lax.dot_general(curve_now, grid_weights, (((0,), (0,)), ((), ())), preferred_element_type=jnp.float32)
            discount = alive_mask * jnp.exp(-yields * remain)
            discounts.append(discount)
            values = values + jnp.dot(discount.astype(jnp.bfloat16), tables[member], preferred_element_type=jnp.float32)
        rooted = jnp.sqrt(values * values + SOFTEN)
        exposure_rows.append(lax.optimization_barrier(jnp.sum(0.5 * (values + rooted), axis=0)) / total_paths)
        slopes = (default_weight[date_index] / total_paths * 0.5 * (1.0 + values / rooted)).astype(jnp.bfloat16)
        group_sens = []
        for member in range(N_CCY):
            back_flow = lax.dot_general(slopes, tables[member], (((1,), (1,)), ((), ())), preferred_element_type=jnp.float32)
            node_pull = lax.optimization_barrier(jnp.sum(back_flow * -remain * discounts[member], axis=0))
            group_sens.append(jnp.dot(weights, node_pull, precision=lax.Precision.HIGHEST))
        sens_rows.append(jnp.stack(group_sens))
    return (jnp.stack(exposure_rows), jnp.stack(sens_rows, axis=1))
```

```python
import functools
import math

import jax
import jax.numpy as jnp
from jax import lax
from jax.experimental import pallas as pl
from jax.experimental.pallas import tpu as pltpu
from jax.sharding import PartitionSpec as P

CFG = 1024
NSETS = 512
SOFTEN = 0.04
HORIZON = 32.0
LOG2E = math.log2(math.e)
VMEM_LIMIT = 56 * 1024 * 1024

NT = (((1,), (1,)), ((), ()))
NN = (((1,), (0,)), ((), ()))


def dot32(a, b, dims):
    return lax.dot_general(a, b, dims, preferred_element_type=jnp.float32)


def table_kernel(idx_ref, amt_ref, set_ref, out_ref, idx_t, hi_t, lo_t, flow_ref, set_oh):
    ncf, trades = idx_ref.shape
    nsets, cfg = out_ref.shape
    sub, lanes, rows = 16, 128, 64
    idx = idx_ref[...]
    total = jnp.zeros((ncf, trades), jnp.float32)
    for k in range(ncf):
        same = idx == idx_ref[k : k + 1, :]
        total = total + jnp.where(same, amt_ref[k : k + 1, :], 0.0)
    high = total.astype(jnp.bfloat16).astype(jnp.float32)
    low = total - high
    for k in range(ncf):
        row = slice(k * sub, (k + 1) * sub)
        shape = (sub, trades)
        idx_t[row, :] = jnp.broadcast_to(idx[k : k + 1, :], shape).astype(jnp.int16)
        hi_t[row, :] = jnp.broadcast_to(high[k : k + 1, :], shape).astype(jnp.bfloat16)
        lo_t[row, :] = jnp.broadcast_to(low[k : k + 1, :], shape).astype(jnp.bfloat16)
    set_rows = lax.broadcasted_iota(jnp.int32, (nsets, trades), 0)
    one_hot = jnp.where(set_rows == set_ref[...], 1.0, 0.0).astype(jnp.bfloat16)
    set_oh[:, :trades] = one_hot
    set_oh[:, trades:] = one_hot

    tiles = rows // sub
    base = lax.broadcasted_iota(jnp.int32, (tiles, sub, lanes), 0) * sub
    base = base + lax.broadcasted_iota(jnp.int32, (tiles, sub, lanes), 1)

    def fill(step, carry):
        block = step // (cfg // rows)
        c0 = (step % (cfg // rows)) * rows
        cols = pl.ds(pl.multiple_of(block * lanes, lanes), lanes)
        lcols = pl.ds(pl.multiple_of(trades + block * lanes, lanes), lanes)
        dates = (base + c0).astype(jnp.int16)
        acc_hi = jnp.zeros((tiles, sub, lanes), jnp.bfloat16)
        acc_lo = jnp.zeros((tiles, sub, lanes), jnp.bfloat16)
        for k in range(ncf):
            row = slice(k * sub, (k + 1) * sub)
            hit = dates == idx_t[row, cols][None]
            acc_hi = jnp.where(hit, hi_t[row, cols][None], acc_hi)
            acc_lo = jnp.where(hit, lo_t[row, cols][None], acc_lo)
        out_rows = pl.ds(pl.multiple_of(c0, rows), rows)
        flow_ref[out_rows, cols] = acc_hi.reshape(rows, lanes)
        flow_ref[out_rows, lcols] = acc_lo.reshape(rows, lanes)
        return carry

    lax.fori_loop(0, (trades // lanes) * (cfg // rows), fill, 0)
    half = 256
    for c0 in range(0, cfg, half):
        block = dot32(set_oh[...], flow_ref[c0 : c0 + half, :], NT)
        out_ref[:, c0 : c0 + half] = block.astype(jnp.bfloat16)


def build_table(idx, amt, sets):
    ncf, trades = idx.shape
    return pl.pallas_call(
        table_kernel,
        out_shape=jax.ShapeDtypeStruct((NSETS, CFG), jnp.bfloat16),
        in_specs=[pl.BlockSpec(memory_space=pltpu.VMEM)] * 3,
        out_specs=pl.BlockSpec(memory_space=pltpu.VMEM),
        scratch_shapes=[
            pltpu.VMEM((ncf * 16, trades), jnp.int16),
            pltpu.VMEM((ncf * 16, trades), jnp.bfloat16),
            pltpu.VMEM((ncf * 16, trades), jnp.bfloat16),
            pltpu.VMEM((CFG, 2 * trades), jnp.bfloat16),
            pltpu.VMEM((NSETS, 2 * trades), jnp.bfloat16),
        ],
        cost_estimate=pl.CostEstimate(
            flops=4 * trades * NSETS * CFG, bytes_accessed=2**21, transcendentals=0
        ),
        compiler_params=pltpu.CompilerParams(vmem_limit_bytes=VMEM_LIMIT),
        name="table",
    )(idx, amt, sets)


def disc_kernel(date_ref, *refs):
    groups = (len(refs) - 3) // 1
    curves, (disc_ref, scaled_ref, rhs) = refs[: len(refs) - 3], refs[len(refs) - 3 :]
    slots, nodes, paths = curves[0].shape
    cfg = disc_ref.shape[2]
    depth = rhs.shape[0]
    for k in range(slots):
        date = date_ref[k]
        start = 0.5 * (date.astype(jnp.float32) + 1.0)
        grid = lax.broadcasted_iota(jnp.int32, (cfg, nodes), 0).astype(jnp.float32)
        remain = HORIZON * (grid + 1.0) / cfg - start
        node = lax.broadcasted_iota(jnp.int32, (cfg, nodes), 1).astype(jnp.float32)
        tenor = HORIZON * (node + 1.0) / nodes
        clipped = jnp.clip(remain, HORIZON / nodes, HORIZON)
        weight = jnp.maximum(0.0, 1.0 - jnp.abs(clipped - tenor) * (nodes / HORIZON))
        scaled = weight * (remain * (-LOG2E))
        scaled_ref[k] = weight * -remain
        high = scaled.astype(jnp.bfloat16)
        rest = scaled - high.astype(jnp.float32)
        mid = rest.astype(jnp.bfloat16)
        low = (rest - mid.astype(jnp.float32)).astype(jnp.bfloat16)
        column = lax.broadcasted_iota(jnp.int32, (cfg, depth - 3 * nodes), 1)
        late = lax.broadcasted_iota(jnp.int32, (cfg, depth - 3 * nodes), 0)
        late = HORIZON * (late.astype(jnp.float32) + 1.0) / cfg - start
        dead = jnp.where((column == 0) & (late <= 0.0), -1e30, 0.0).astype(jnp.bfloat16)
        lhs = jnp.concatenate([high, mid, low, dead], axis=1)
        for g in range(groups):
            part = curves[g][k]
            for copy in range(3):
                rhs[copy * nodes : (copy + 1) * nodes, :] = part
            rhs[3 * nodes :, :] = jnp.ones((depth - 3 * nodes, paths), jnp.bfloat16)
            disc_ref[k, g] = jnp.exp2(dot32(lhs, rhs[...], NN)).astype(jnp.bfloat16)


def discounts(dates, curves):
    slots, nodes, paths = curves[0].shape
    groups = len(curves)
    return pl.pallas_call(
        disc_kernel,
        out_shape=(
            jax.ShapeDtypeStruct((slots, groups, CFG, paths), jnp.bfloat16),
            jax.ShapeDtypeStruct((slots, CFG, nodes), jnp.float32),
        ),
        in_specs=[pl.BlockSpec(memory_space=pltpu.SMEM)]
        + [pl.BlockSpec(memory_space=pltpu.VMEM)] * groups,
        out_specs=(pl.BlockSpec(memory_space=pltpu.VMEM),) * 2,
        scratch_shapes=[pltpu.VMEM((4 * nodes, paths), jnp.bfloat16)],
        cost_estimate=pl.CostEstimate(
            flops=2 * slots * groups * CFG * paths * 4 * nodes,
            bytes_accessed=2 * slots * groups * CFG * paths,
            transcendentals=slots * groups * CFG * paths,
        ),
        compiler_params=pltpu.CompilerParams(vmem_limit_bytes=VMEM_LIMIT),
        name="discounts",
    )(dates, *curves)


def price_kernel(scale, weight_ref, scaled_ref, disc_ref, *refs):
    groups = disc_ref.shape[1]
    tables = refs[:groups]
    expo_ref, sens_ref, value_ref, slope_ref, pull_ref = refs[groups:]
    slots = disc_ref.shape[0]
    nsets, cfg = tables[0].shape
    paths = disc_ref.shape[3]
    lanes = 128
    for k in range(slots):
        value = dot32(tables[0][...], disc_ref[k, 0], NN)
        for g in range(1, groups):
            value = value + dot32(tables[g][...], disc_ref[k, g], NN)
        square = value * value + SOFTEN
        inverse = lax.rsqrt(square)
        positive = 0.5 * (value + square * inverse)
        folded = positive[:, :lanes]
        for p0 in range(lanes, paths, lanes):
            folded = folded + positive[:, p0 : p0 + lanes]
        ones = jnp.ones((8, lanes), jnp.float32)
        summed = lax.dot_general(
            ones, folded, NT, precision=lax.Precision.HIGHEST, preferred_element_type=jnp.float32
        )
        expo_ref[k : k + 1, :] = summed[0:1] * scale
        row = weight_ref[k][:, :1] * (0.5 * scale)
        slope_ref[...] = (row * (1.0 + value * inverse)).astype(jnp.bfloat16)
        pull_ref[...] = jnp.zeros_like(pull_ref)
        for g in range(groups):
            back = dot32(slope_ref[...], disc_ref[k, g], NT)
            weighted = back * tables[g][...].astype(jnp.float32)
            pull_ref[g : g + 1, :] = jnp.sum(weighted, axis=0, keepdims=True)
        sens = lax.dot_general(
            pull_ref[...], scaled_ref[k], NN,
            precision=lax.Precision.HIGHEST, preferred_element_type=jnp.float32,
        )
        sens_ref[k] = sens[:groups]


def price(weights, scaled, disc, tables, total_paths):
    slots, groups, cfg, paths = disc.shape
    nodes = scaled.shape[2]
    rows = -(-groups // 8) * 8
    return pl.pallas_call(
        functools.partial(price_kernel, 1.0 / total_paths),
        out_shape=(
            jax.ShapeDtypeStruct((slots, NSETS), jnp.float32),
            jax.ShapeDtypeStruct((slots, groups, nodes), jnp.float32),
        ),
        in_specs=[pl.BlockSpec(memory_space=pltpu.VMEM)] * (3 + groups),
        out_specs=(pl.BlockSpec(memory_space=pltpu.VMEM),) * 2,
        scratch_shapes=[
            pltpu.VMEM((NSETS, paths), jnp.float32),
            pltpu.VMEM((NSETS, paths), jnp.bfloat16),
            pltpu.VMEM((rows, CFG), jnp.float32),
        ],
        cost_estimate=pl.CostEstimate(
            flops=4 * slots * groups * CFG * paths * NSETS,
            bytes_accessed=2 * slots * groups * CFG * paths,
            transcendentals=slots * NSETS * paths,
        ),
        compiler_params=pltpu.CompilerParams(vmem_limit_bytes=VMEM_LIMIT),
        name="price",
    )(weights, scaled, disc, *tables)


def local(curve_store, cash_index, cash_amount, trade_set, date_slot, default_weight):
    groups = lax.axis_size("ccy")
    stations = lax.axis_size("path")
    group_index = lax.axis_index("ccy")
    station = lax.axis_index("path")
    dates = date_slot.shape[0]
    _, slots, nodes, total_paths = curve_store.shape
    paths = total_paths // groups
    share = NSETS // groups

    def swap(array, mask):
        return lax.ppermute(array, "ccy", [(i, i ^ mask) for i in range(groups)])

    flows = (jnp.swapaxes(cash_index[0], 0, 1), jnp.swapaxes(cash_amount[0], 0, 1), trade_set)
    others = {m: tuple(swap(part, m) for part in flows) for m in range(2, groups, 2)}

    def piece(mask):
        begin = (group_index ^ mask) * paths
        return lax.dynamic_slice_in_dim(curve_store[0], begin, paths, 2)

    curves = [piece(0)] + [swap(piece(m), m) for m in range(1, groups)]

    tables = {0: build_table(*flows)}
    for m in others:
        tables[m] = build_table(*others[m])
    for m in list(tables):
        tables[m + 1] = swap(tables[m], 1)
    tables = [tables[m] for m in range(groups)]

    slot_ids = station * slots + jnp.arange(slots, dtype=jnp.int32)
    match = date_slot[None, :] == slot_ids[:, None]
    date_ids = jnp.sum(jnp.where(match, jnp.arange(dates, dtype=jnp.int32)[None, :], 0), axis=1)
    weights = jnp.sum(jnp.where(match[:, :, None], default_weight[None], 0.0), axis=1)
    weights = jnp.broadcast_to(weights[:, :, None], (slots, NSETS, 128))

    disc, scaled = discounts(date_ids, curves)
    expo, sens = price(weights, scaled, disc, tables, total_paths)

    expo = jnp.swapaxes(expo.reshape(slots, groups, share), 0, 1)
    order = group_index ^ jnp.arange(groups)
    pick = (order[:, None] == jnp.arange(groups)[None, :]).astype(jnp.float32)
    sens = jnp.sum(pick[:, :, None, None] * jnp.swapaxes(sens, 0, 1)[None], axis=1)
    payload = jnp.concatenate([expo, sens], axis=2)
    payload = jnp.broadcast_to(payload[:, None], (groups, stations, slots, share + nodes))
    payload = payload.reshape(groups * stations, slots * (share + nodes))
    payload = lax.all_to_all(payload, ("ccy", "path"), 0, 0, tiled=True)
    summed = jnp.sum(payload.reshape(groups, stations * slots, share + nodes), axis=0)
    chosen = (date_slot[:, None] == jnp.arange(stations * slots)[None, :]).astype(jnp.float32)
    rows = jnp.dot(chosen, summed, precision=lax.Precision.HIGHEST)
    return rows[:, :share], rows[:, share:][None]


def solution(mesh):
    in_specs = (
        P("ccy", "path", None, None),
        P("ccy", None, None),
        P("ccy", None, None),
        P("ccy", None),
        P(),
        P(),
    )
    out_specs = (P(None, "ccy"), P("ccy", None, None))
    return jax.shard_map(local, mesh=mesh, in_specs=in_specs, out_specs=out_specs, check_vma=False)
```

```python
import functools
import math

import jax
import jax.numpy as jnp
from jax import lax
from jax.experimental import pallas as pl
from jax.experimental.pallas import tpu as pltpu
from jax.sharding import PartitionSpec as P


CFG = 1024
NSETS = 512
SOFTEN = 0.04
HORIZON = 32.0
LOG2E = math.log2(math.e)
LANES = 128
SUB = 16
WIDE = 256

NT = (((1,), (1,)), ((), ()))
NN = (((1,), (0,)), ((), ()))
TN = (((0,), (0,)), ((), ()))
VM = pl.BlockSpec(memory_space=pltpu.VMEM)
SM = pl.BlockSpec(memory_space=pltpu.SMEM)


def dot16(a, b, dims):
    return lax.dot_general(a, b, dims, preferred_element_type=jnp.float32)


def dot_full(a, b, dims):
    return lax.dot_general(
        a, b, dims, precision=lax.Precision.HIGHEST, preferred_element_type=jnp.float32
    )


def join(ref, blocks):
    return jnp.concatenate([ref[b] for b in blocks], axis=1)


def table_kernel(flow_ref, out_ref, date_t, high_t, one_hot, slot_a, slot_b, acc_ref):
    ncf, trades = flow_ref.shape[0] // 2, flow_ref.shape[1]
    blocks = trades // LANES
    row_ids = lax.broadcasted_iota(jnp.int32, (NSETS // SUB, SUB, LANES), 0) * SUB
    row_ids = (row_ids + lax.broadcasted_iota(jnp.int32, row_ids.shape, 1)).astype(jnp.int16)
    unit = jnp.ones((NSETS // SUB, SUB, LANES), jnp.bfloat16)

    def spread(row):
        return jnp.broadcast_to(row, (SUB, LANES))

    def prepare(b, carry):
        cols = pl.ds(pl.multiple_of(b * LANES, LANES), LANES)
        code = flow_ref[:ncf, cols].astype(jnp.int32)
        amount = flow_ref[ncf:, cols]
        date = code & (CFG - 1)
        sets = lax.shift_right_logical(code[0:1, :], CFG.bit_length() - 1)
        total = jnp.zeros((ncf, LANES), jnp.float32)
        for k in range(ncf):
            same = date == date[k : k + 1, :]
            total = total + jnp.where(same, amount[k : k + 1, :], 0.0)
        for k in range(ncf):
            rows = slice(k * SUB, (k + 1) * SUB)
            date_t[b, rows, :] = spread(date[k : k + 1, :]).astype(jnp.int16)
            high_t[b, rows, :] = spread(total[k : k + 1, :]).astype(jnp.bfloat16)
        mine = spread(sets).astype(jnp.int16)[None]
        chosen = jnp.where(row_ids == mine, unit, jnp.zeros_like(unit))
        one_hot[b] = chosen.reshape(NSETS, LANES)
        return carry

    lax.fori_loop(0, blocks, prepare, 0)

    chunk, tiles = 8, 8
    step = tiles * SUB
    parts = CFG // WIDE
    base = lax.broadcasted_iota(jnp.int32, (tiles, SUB, LANES), 0) * SUB
    base = base + lax.broadcasted_iota(jnp.int32, (tiles, SUB, LANES), 1)
    slots = (slot_a, slot_b)

    def fill(slot, part, b):
        for r in range(0, WIDE, step):
            want = (base + (part * WIDE + r)).astype(jnp.int16)
            acc = jnp.zeros((tiles, SUB, LANES), jnp.bfloat16)
            for k in range(ncf):
                rows = slice(k * SUB, (k + 1) * SUB)
                acc = jnp.where(want == date_t[b, rows, :][None], high_t[b, rows, :][None], acc)
            slot[b, r : r + step, :] = acc.reshape(step, LANES)

    for part in range(parts + 1):
        target, source = slots[part % 2], slots[(part + 1) % 2]
        if part > 0:
            acc_ref[...] = jnp.zeros_like(acc_ref)

        def body(q, carry, part=part, target=target, source=source):
            mine = [q * chunk + i for i in range(chunk)]
            if part > 0:
                acc_ref[...] += dot16(join(one_hot, mine), join(source, mine), NT)
            if part < parts:
                for b in mine:
                    fill(target, part, b)
            return carry

        lax.fori_loop(0, blocks // chunk, body, 0)
        if part > 0:
            block = acc_ref[...].astype(jnp.bfloat16)
            for i in range(WIDE // LANES):
                place = (part - 1) * (WIDE // LANES) + i
                out_ref[place] = block[:, i * LANES : (i + 1) * LANES]


def build_table(flows):
    ncf, trades = flows.shape[0] // 2, flows.shape[1]
    blocks = trades // LANES
    return pl.pallas_call(
        table_kernel,
        out_shape=jax.ShapeDtypeStruct((CFG // LANES, NSETS, LANES), jnp.bfloat16),
        in_specs=[VM],
        out_specs=VM,
        scratch_shapes=[
            pltpu.VMEM((blocks, ncf * SUB, LANES), jnp.int16),
            pltpu.VMEM((blocks, ncf * SUB, LANES), jnp.bfloat16),
            pltpu.VMEM((blocks, NSETS, LANES), jnp.bfloat16),
            pltpu.VMEM((blocks, WIDE, LANES), jnp.bfloat16),
            pltpu.VMEM((blocks, WIDE, LANES), jnp.bfloat16),
            pltpu.VMEM((NSETS, WIDE), jnp.float32),
        ],
        cost_estimate=pl.CostEstimate(
            flops=4 * trades * NSETS * CFG, bytes_accessed=2**21, transcendentals=0
        ),
        compiler_params=pltpu.CompilerParams(vmem_limit_bytes=16 * 2**20),
    )(flows)


def date_of(slot_ref, station_ref, slots, k):
    mine = station_ref[0] * slots + k
    date, found = 0, 0
    for d in range(slot_ref.shape[0]):
        hit = slot_ref[d] == mine
        date = jnp.where(hit, d, date)
        found = jnp.where(hit, 1, found)
    return date, found


def disc_kernel(groups, slot_ref, station_ref, *refs):
    curves, (disc_ref, scaled_ref, rhs) = refs[:groups], refs[groups:]
    slots, nodes, paths = curves[0].shape
    depth = rhs.shape[0]
    rhs[3 * nodes :, :] = jnp.ones((depth - 3 * nodes, paths), jnp.bfloat16)
    for k in range(slots):
        date, _ = date_of(slot_ref, station_ref, slots, k)
        start = 0.5 * (date.astype(jnp.float32) + 1.0)
        grid = lax.broadcasted_iota(jnp.int32, (CFG, nodes), 0).astype(jnp.float32)
        remain = HORIZON * (grid + 1.0) / CFG - start
        node = lax.broadcasted_iota(jnp.int32, (CFG, nodes), 1).astype(jnp.float32)
        tenor = HORIZON * (node + 1.0) / nodes
        clipped = jnp.clip(remain, HORIZON / nodes, HORIZON)
        weight = jnp.maximum(0.0, 1.0 - jnp.abs(clipped - tenor) * (nodes / HORIZON))
        scaled = weight * (remain * (-LOG2E))
        scaled_ref[k] = weight * -remain
        high = scaled.astype(jnp.bfloat16)
        rest = scaled - high.astype(jnp.float32)
        mid = rest.astype(jnp.bfloat16)
        low = (rest - mid.astype(jnp.float32)).astype(jnp.bfloat16)
        dead = jnp.where((node == 0.0) & (remain <= 0.0), -1e30, 0.0).astype(jnp.bfloat16)
        left = jnp.concatenate([high, mid, low, dead], axis=1)
        for g in range(groups):
            part = curves[g][k]
            for copy in range(3):
                rhs[copy * nodes : (copy + 1) * nodes, :] = part
            for p0 in range(0, paths, WIDE):
                block = jnp.exp2(dot16(left, rhs[:, p0 : p0 + WIDE], NN)).astype(jnp.bfloat16)
                for i in range(WIDE // LANES):
                    disc_ref[k, g, p0 // LANES + i] = block[:, i * LANES : (i + 1) * LANES]


def discounts(date_slot, station, curves):
    slots, nodes, paths = curves[0].shape
    groups = len(curves)
    return pl.pallas_call(
        functools.partial(disc_kernel, groups),
        out_shape=(
            jax.ShapeDtypeStruct((slots, groups, paths // LANES, CFG, LANES), jnp.bfloat16),
            jax.ShapeDtypeStruct((slots, CFG, nodes), jnp.float32),
        ),
        in_specs=[SM, SM] + [VM] * groups,
        out_specs=(VM, VM),
        scratch_shapes=[pltpu.VMEM((4 * nodes, paths), jnp.bfloat16)],
        cost_estimate=pl.CostEstimate(
            flops=2 * slots * groups * CFG * paths * 4 * nodes,
            bytes_accessed=2 * slots * groups * CFG * paths,
            transcendentals=slots * groups * CFG * paths,
        ),
        compiler_params=pltpu.CompilerParams(
            vmem_limit_bytes=8 * 2**20 + 3 * slots * groups * CFG * paths
        ),
        name="discounts",
    )(date_slot, station, *curves)


def price_kernel(stations, scale, slot_ref, station_ref, member_ref, weight_ref, scaled_ref,
                 disc_ref, *refs):
    groups = disc_ref.shape[1]
    tables = refs[:groups]
    out_ref, slope_ref, expo_ref, pull_ref, sens_ref = refs[groups:]
    slots = disc_ref.shape[0]
    pblocks = disc_ref.shape[2]
    cblocks = CFG // LANES
    nodes = scaled_ref.shape[2]
    share = NSETS // groups
    wide = WIDE // LANES
    lead = (lax.broadcasted_iota(jnp.int32, (8, LANES), 0) == 0).astype(jnp.float32)
    pull_ref[...] = jnp.zeros_like(pull_ref)
    for k in range(slots):
        date, found = date_of(slot_ref, station_ref, slots, k)
        row = weight_ref[pl.ds(date, 1), :] * (0.5 * scale) * found.astype(jnp.float32)
        column = dot_full(jnp.broadcast_to(row, (8, NSETS)), lead, TN)
        folded = jnp.zeros((NSETS, LANES), jnp.float32)
        left = jnp.concatenate([join(tables[g], range(cblocks)) for g in range(groups)], axis=1)
        for p0 in range(0, pblocks, wide):
            right = jnp.concatenate(
                [join(disc_ref.at[k, g], range(p0, p0 + wide)) for g in range(groups)], axis=0
            )
            value = dot16(left, right, NN)
            for i in range(wide):
                part = value[:, i * LANES : (i + 1) * LANES]
                square = part * part + SOFTEN
                inverse = lax.rsqrt(square)
                folded = folded + (part + square * inverse)
                slope = column + column * (part * inverse)
                slope_ref[p0 + i] = slope.astype(jnp.bfloat16)
        summed = dot_full(jnp.ones((8, LANES), jnp.float32), folded, NT)
        expo_ref[k : k + 1, :] = summed[0:1] * (0.5 * scale)
        slope_all = join(slope_ref, range(pblocks))
        for g in range(groups):
            for c0 in range(0, cblocks, wide):
                right = jnp.concatenate(
                    [disc_ref[k, g, p, c0 * LANES : (c0 + wide) * LANES, :] for p in range(pblocks)],
                    axis=1,
                )
                back = dot16(slope_all, right, NT)
                for i in range(wide):
                    cash = tables[g][c0 + i].astype(jnp.float32)
                    pull = jnp.sum(back[:, i * LANES : (i + 1) * LANES] * cash, axis=0)
                    cols = slice((c0 + i) * LANES, (c0 + i + 1) * LANES)
                    pull_ref[g : g + 1, cols] = pull[None]
        sens_ref[k] = dot_full(pull_ref[...], scaled_ref[k], NN)
    for g in range(groups):
        rows = slice(g * stations, (g + 1) * stations)
        mask = member_ref[0] ^ g
        for k in range(slots):
            part = expo_ref[k : k + 1, g * share : (g + 1) * share]
            out_ref[rows, k * share : (k + 1) * share] = jnp.broadcast_to(part, (stations, share))
        line = jnp.concatenate([sens_ref[k, pl.ds(mask, 1), :] for k in range(slots)], axis=1)
        out_ref[rows, slots * share :] = jnp.broadcast_to(line, (stations, slots * nodes))


def price(date_slot, station, member, weights, scaled, disc, tables, stations, total_paths):
    slots, groups, pblocks = disc.shape[:3]
    nodes = scaled.shape[2]
    paths = pblocks * LANES
    rows = -(-groups // 8) * 8
    return pl.pallas_call(
        functools.partial(price_kernel, stations, 1.0 / total_paths),
        out_shape=jax.ShapeDtypeStruct(
            (groups * stations, slots * (NSETS // groups + nodes)), jnp.float32
        ),
        in_specs=[SM] * 3 + [VM] * (3 + groups),
        out_specs=VM,
        scratch_shapes=[
            pltpu.VMEM((pblocks, NSETS, LANES), jnp.bfloat16),
            pltpu.VMEM((slots, NSETS), jnp.float32),
            pltpu.VMEM((rows, CFG), jnp.float32),
            pltpu.VMEM((slots, rows, nodes), jnp.float32),
        ],
        cost_estimate=pl.CostEstimate(
            flops=4 * slots * groups * CFG * paths * NSETS,
            bytes_accessed=2 * slots * groups * CFG * paths,
            transcendentals=slots * NSETS * paths,
        ),
        compiler_params=pltpu.CompilerParams(
            vmem_limit_bytes=16 * 2**20 + 3 * slots * groups * CFG * paths // 2
        ),
        name="price",
    )(date_slot, station, member, weights, scaled, disc, *tables)


def collect_kernel(groups, slots, nodes, slot_ref, got_ref, expo_ref, sens_ref, sum_ref):
    stations = sum_ref.shape[0]
    dates, share = expo_ref.shape
    total = got_ref[:stations]
    for g in range(1, groups):
        total = total + got_ref[g * stations : (g + 1) * stations]
    sum_ref[...] = total
    for d in range(dates):
        slot = slot_ref[d]
        line = sum_ref[pl.ds(slot // slots, 1), :]
        expo, sens = line[:, :share], line[:, slots * share : slots * share + nodes]
        for k in range(1, slots):
            here = slot % slots == k
            begin = slots * share + k * nodes
            expo = jnp.where(here, line[:, k * share : (k + 1) * share], expo)
            sens = jnp.where(here, line[:, begin : begin + nodes], sens)
        expo_ref[d : d + 1, :] = expo
        sens_ref[d : d + 1, :] = sens


def collect(date_slot, got, groups, slots, nodes):
    dates = date_slot.shape[0]
    share = NSETS // groups
    return pl.pallas_call(
        functools.partial(collect_kernel, groups, slots, nodes),
        out_shape=(
            jax.ShapeDtypeStruct((dates, share), jnp.float32),
            jax.ShapeDtypeStruct((dates, nodes), jnp.float32),
        ),
        in_specs=[SM, VM],
        out_specs=(VM, VM),
        scratch_shapes=[pltpu.VMEM((got.shape[0] // groups, got.shape[1]), jnp.float32)],
        name="collect",
    )(date_slot, got)


def local(curve_store, cash_index, cash_amount, trade_set, date_slot, default_weight):
    groups = lax.axis_size("ccy")
    stations = lax.axis_size("path")
    member = lax.axis_index("ccy").astype(jnp.int32)
    station = lax.axis_index("path").astype(jnp.int32)
    _, slots, nodes, total_paths = curve_store.shape
    paths = total_paths // groups

    def swap(array, mask):
        return lax.ppermute(array, "ccy", [(i, i ^ mask) for i in range(groups)])

    code = jnp.swapaxes(cash_index[0], 0, 1) + CFG * trade_set
    flows = jnp.concatenate([code.astype(jnp.float32), jnp.swapaxes(cash_amount[0], 0, 1)], axis=0)
    others = {m: swap(flows, m) for m in range(2, groups, 2)}

    def piece(mask):
        begin = (member ^ mask) * paths
        return lax.dynamic_slice_in_dim(curve_store[0], begin, paths, 2)

    curves = [piece(0)] + [swap(piece(m), m) for m in range(1, groups)]

    tables = {0: build_table(flows)}
    for m in others:
        tables[m] = build_table(others[m])
    for m in list(tables):
        tables[m + 1] = swap(tables[m], 1)
    tables = [tables[m] for m in range(groups)]

    disc, scaled = discounts(date_slot, station[None], curves)
    payload = price(
        date_slot, station[None], member[None], default_weight, scaled, disc, tables,
        stations, total_paths,
    )
    got = lax.all_to_all(payload, ("ccy", "path"), 0, 0, tiled=True)
    expo, sens = collect(date_slot, got, groups, slots, nodes)
    return expo, sens[None]


def solution(mesh):
    in_specs = (
        P("ccy", "path", None, None),
        P("ccy", None, None),
        P("ccy", None, None),
        P("ccy", None),
        P(),
        P(),
    )
    out_specs = (P(None, "ccy"), P("ccy", None, None))
    return jax.shard_map(local, mesh=mesh, in_specs=in_specs, out_specs=out_specs, check_vma=False)
```

```python
import functools
import math

import jax
import jax.numpy as jnp
from jax import lax
from jax.experimental import pallas as pl
from jax.experimental.pallas import tpu as pltpu
from jax.sharding import PartitionSpec as P


CFG = 1024
NSETS = 512
SOFTEN = 0.04
HORIZON = 32.0
LOG2E = math.log2(math.e)
LANES = 128
SUB = 16
WIDE = 256

NT = (((1,), (1,)), ((), ()))
NN = (((1,), (0,)), ((), ()))
TN = (((0,), (0,)), ((), ()))
VM = pl.BlockSpec(memory_space=pltpu.VMEM)


def dot16(a, b, dims):
    return lax.dot_general(a, b, dims, preferred_element_type=jnp.float32)


def dot_full(a, b, dims):
    return lax.dot_general(
        a, b, dims, precision=lax.Precision.HIGHEST, preferred_element_type=jnp.float32
    )


def join(ref, blocks):
    return jnp.concatenate([ref[b] for b in blocks], axis=1)


def table_kernel(flow_ref, out_ref, date_t, high_t, one_hot, slot_a, slot_b, acc_ref):
    ncf, trades = flow_ref.shape[0] // 2, flow_ref.shape[1]
    blocks = trades // LANES
    row_ids = lax.broadcasted_iota(jnp.int32, (NSETS // SUB, SUB, LANES), 0) * SUB
    row_ids = (row_ids + lax.broadcasted_iota(jnp.int32, row_ids.shape, 1)).astype(jnp.int16)
    unit = jnp.ones((NSETS // SUB, SUB, LANES), jnp.bfloat16)

    def spread(row):
        return jnp.broadcast_to(row, (SUB, LANES))

    def prepare(b, carry):
        cols = pl.ds(pl.multiple_of(b * LANES, LANES), LANES)
        code = flow_ref[:ncf, cols].astype(jnp.int32)
        amount = flow_ref[ncf:, cols]
        date = code & (CFG - 1)
        sets = lax.shift_right_logical(code[0:1, :], CFG.bit_length() - 1)
        total = jnp.zeros((ncf, LANES), jnp.float32)
        for k in range(ncf):
            same = date == date[k : k + 1, :]
            total = total + jnp.where(same, amount[k : k + 1, :], 0.0)
        for k in range(ncf):
            rows = slice(k * SUB, (k + 1) * SUB)
            date_t[b, rows, :] = spread(date[k : k + 1, :]).astype(jnp.int16)
            high_t[b, rows, :] = spread(total[k : k + 1, :]).astype(jnp.bfloat16)
        mine = spread(sets).astype(jnp.int16)[None]
        chosen = jnp.where(row_ids == mine, unit, jnp.zeros_like(unit))
        one_hot[b] = chosen.reshape(NSETS, LANES)
        return carry

    lax.fori_loop(0, blocks, prepare, 0)

    chunk, tiles = 8, 8
    step = tiles * SUB
    parts = CFG // WIDE
    base = lax.broadcasted_iota(jnp.int32, (tiles, SUB, LANES), 0) * SUB
    base = base + lax.broadcasted_iota(jnp.int32, (tiles, SUB, LANES), 1)
    slots = (slot_a, slot_b)

    def fill(slot, part, b):
        for r in range(0, WIDE, step):
            want = (base + (part * WIDE + r)).astype(jnp.int16)
            acc = jnp.zeros((tiles, SUB, LANES), jnp.bfloat16)
            for k in range(ncf):
                rows = slice(k * SUB, (k + 1) * SUB)
                acc = jnp.where(want == date_t[b, rows, :][None], high_t[b, rows, :][None], acc)
            slot[b, r : r + step, :] = acc.reshape(step, LANES)

    for part in range(parts + 1):
        target, source = slots[part % 2], slots[(part + 1) % 2]
        if part > 0:
            acc_ref[...] = jnp.zeros_like(acc_ref)

        def body(q, carry, part=part, target=target, source=source):
            mine = [q * chunk + i for i in range(chunk)]
            if part > 0:
                acc_ref[...] += dot16(join(one_hot, mine), join(source, mine), NT)
            if part < parts:
                for b in mine:
                    fill(target, part, b)
            return carry

        lax.fori_loop(0, blocks // chunk, body, 0)
        if part > 0:
            block = acc_ref[...].astype(jnp.bfloat16)
            for i in range(WIDE // LANES):
                place = (part - 1) * (WIDE // LANES) + i
                out_ref[place] = block[:, i * LANES : (i + 1) * LANES]


def build_table(flows):
    ncf, trades = flows.shape[0] // 2, flows.shape[1]
    blocks = trades // LANES
    return pl.pallas_call(
        table_kernel,
        out_shape=jax.ShapeDtypeStruct((CFG // LANES, NSETS, LANES), jnp.bfloat16),
        in_specs=[VM],
        out_specs=VM,
        scratch_shapes=[
            pltpu.VMEM((blocks, ncf * SUB, LANES), jnp.int16),
            pltpu.VMEM((blocks, ncf * SUB, LANES), jnp.bfloat16),
            pltpu.VMEM((blocks, NSETS, LANES), jnp.bfloat16),
            pltpu.VMEM((blocks, WIDE, LANES), jnp.bfloat16),
            pltpu.VMEM((blocks, WIDE, LANES), jnp.bfloat16),
            pltpu.VMEM((NSETS, WIDE), jnp.float32),
        ],
        cost_estimate=pl.CostEstimate(
            flops=4 * trades * NSETS * CFG, bytes_accessed=2**21, transcendentals=0
        ),
        compiler_params=pltpu.CompilerParams(vmem_limit_bytes=12 * 2**20),
    )(flows)


def prepare_kernel(groups, stations, scale, *refs):
    sources, outs, scratch = refs[:6], refs[6 : 12 + groups], refs[12 + groups :]
    flow_ref, left_ref, scaled_ref, column_ref, pick_ref, route_ref, *pieces = outs
    copies = [
        pltpu.make_async_copy(source, held, scratch[6].at[i])
        for i, (source, held) in enumerate(zip(sources, scratch[:6]))
    ]
    for copy in copies:
        copy.start()
    for copy in copies:
        copy.wait()
    index_ref, amount_ref, set_ref, curve_ref, weight_ref, slot_ref = scratch[:6]
    ncf = index_ref.shape[0]
    slots, nodes, total_paths = curve_ref.shape
    paths = total_paths // groups
    dates = slot_ref.shape[0]
    station, member = lax.axis_index("path"), lax.axis_index("ccy")
    code = index_ref[...] + CFG * set_ref[...]
    flow_ref[:ncf, :] = code.astype(jnp.float32)
    flow_ref[ncf:, :] = amount_ref[...]
    for mask, piece in enumerate(pieces):
        begin = pl.multiple_of((member ^ mask) * paths, LANES)
        for k in range(slots):
            piece[k] = curve_ref[k, :, pl.ds(begin, paths)]
    lead = (lax.broadcasted_iota(jnp.int32, (8, LANES), 0) == 0).astype(jnp.float32)
    for k in range(slots):
        date, found = 0, 0
        for d in range(dates):
            hit = slot_ref[d] == station * slots + k
            date = jnp.where(hit, d, date)
            found = jnp.where(hit, 1, found)
        row = weight_ref[pl.ds(date, 1), :] * (0.5 * scale) * found.astype(jnp.float32)
        column_ref[k] = dot_full(jnp.broadcast_to(row, (8, NSETS)), lead, TN)
        start = 0.5 * (date.astype(jnp.float32) + 1.0)
        grid = lax.broadcasted_iota(jnp.int32, (CFG, nodes), 0).astype(jnp.float32)
        remain = HORIZON * (grid + 1.0) / CFG - start
        node = lax.broadcasted_iota(jnp.int32, (CFG, nodes), 1).astype(jnp.float32)
        tenor = HORIZON * (node + 1.0) / nodes
        clipped = jnp.clip(remain, HORIZON / nodes, HORIZON)
        weight = jnp.maximum(0.0, 1.0 - jnp.abs(clipped - tenor) * (nodes / HORIZON))
        scaled = weight * (remain * (-LOG2E))
        scaled_ref[k] = weight * -remain
        high = scaled.astype(jnp.bfloat16)
        rest = scaled - high.astype(jnp.float32)
        mid = rest.astype(jnp.bfloat16)
        low = (rest - mid.astype(jnp.float32)).astype(jnp.bfloat16)
        dead = jnp.where((node == 0.0) & (remain <= 0.0), -1e30, 0.0).astype(jnp.bfloat16)
        left = jnp.concatenate([high, mid, low, dead], axis=1)
        for i in range(4 * nodes // LANES):
            left_ref[k, i] = left[:, i * LANES : (i + 1) * LANES]
    line = lax.broadcasted_iota(jnp.int32, (dates, LANES), 0)
    slot_of = jnp.zeros((dates, LANES), jnp.int32)
    for d in range(dates):
        slot_of = jnp.where(line == d, slot_ref[d], slot_of)
    for i in range(stations * slots):
        pick_ref[i] = (slot_of == i).astype(jnp.float32)
    for g in range(groups):
        for m in range(groups):
            chosen = ((member ^ g) == m).astype(jnp.float32)
            route_ref[g * groups + m] = jnp.full((8, LANES), chosen, jnp.float32)


def prepare(date_slot, index, amount, sets, curve, weights, groups, stations):
    ncf, trades = index.shape
    slots, nodes, total_paths = curve.shape
    dates = date_slot.shape[0]
    sources = (index, amount, sets, curve, weights, date_slot)
    return pl.pallas_call(
        functools.partial(prepare_kernel, groups, stations, 1.0 / total_paths),
        out_shape=(
            jax.ShapeDtypeStruct((2 * ncf, trades), jnp.float32),
            jax.ShapeDtypeStruct((slots, 4 * nodes // LANES, CFG, LANES), jnp.bfloat16),
            jax.ShapeDtypeStruct((slots, CFG, nodes), jnp.float32),
            jax.ShapeDtypeStruct((slots, NSETS, LANES), jnp.float32),
            jax.ShapeDtypeStruct((stations * slots, dates, LANES), jnp.float32),
            jax.ShapeDtypeStruct((groups * groups, 8, LANES), jnp.float32),
        )
        + (jax.ShapeDtypeStruct((slots, nodes, total_paths // groups), jnp.bfloat16),) * groups,
        in_specs=[pl.BlockSpec(memory_space=pltpu.HBM)] * 6,
        out_specs=(VM,) * (6 + groups),
        scratch_shapes=[pltpu.VMEM(source.shape, source.dtype) for source in sources[:5]]
        + [pltpu.SMEM((dates,), jnp.int32), pltpu.SemaphoreType.DMA((6,))],
        cost_estimate=pl.CostEstimate(flops=2**22, bytes_accessed=2**21, transcendentals=0),
        compiler_params=pltpu.CompilerParams(
            vmem_limit_bytes=14 * 2**20 + 6 * slots * nodes * total_paths
        ),
        name="prepare",
    )(*[pltpu.with_memory_space_constraint(source, pltpu.HBM) for source in sources])


def grant(own, shared):
    return own if shared <= 2**24 else 62 * 2**20


def disc_kernel(groups, left_ref, *refs):
    curves, (disc_ref, rhs) = refs[:groups], refs[groups:]
    slots, nodes, paths = curves[0].shape
    depth = rhs.shape[0]
    rhs[3 * nodes :, :] = jnp.ones((depth - 3 * nodes, paths), jnp.bfloat16)
    for k in range(slots):
        left = join(left_ref.at[k], range(depth // LANES))
        for g in range(groups):
            for copy in range(3):
                rhs[copy * nodes : (copy + 1) * nodes, :] = curves[g][k]
            for p0 in range(0, paths, WIDE):
                block = jnp.exp2(dot16(left, rhs[:, p0 : p0 + WIDE], NN)).astype(jnp.bfloat16)
                for i in range(WIDE // LANES):
                    disc_ref[k, g, p0 // LANES + i] = block[:, i * LANES : (i + 1) * LANES]


def discounts(left, curves):
    slots, nodes, paths = curves[0].shape
    groups = len(curves)
    return pl.pallas_call(
        functools.partial(disc_kernel, groups),
        out_shape=jax.ShapeDtypeStruct(
            (slots, groups, paths // LANES, CFG, LANES), jnp.bfloat16
        ),
        in_specs=[VM] * (1 + groups),
        out_specs=VM,
        scratch_shapes=[pltpu.VMEM((4 * nodes, paths), jnp.bfloat16)],
        cost_estimate=pl.CostEstimate(
            flops=2 * slots * groups * CFG * paths * 4 * nodes,
            bytes_accessed=2 * slots * groups * CFG * paths,
            transcendentals=slots * groups * CFG * paths,
        ),
        compiler_params=pltpu.CompilerParams(
            vmem_limit_bytes=grant(6 * 2**20, 2 * slots * groups * CFG * paths)
        ),
        name="discounts",
    )(left, *curves)


def price_kernel(stations, scale, column_ref, scaled_ref, route_ref, disc_ref, *refs):
    groups = disc_ref.shape[1]
    tables = refs[:groups]
    out_ref, slope_ref, expo_ref, pull_ref, sens_ref = refs[groups:]
    slots = disc_ref.shape[0]
    pblocks = disc_ref.shape[2]
    cblocks = CFG // LANES
    nodes = scaled_ref.shape[2]
    share = NSETS // groups
    wide = WIDE // LANES
    pull_ref[...] = jnp.zeros_like(pull_ref)
    for k in range(slots):
        column = column_ref[k]
        folded = jnp.zeros((NSETS, LANES), jnp.float32)
        left = jnp.concatenate([join(tables[g], range(cblocks)) for g in range(groups)], axis=1)
        for p0 in range(0, pblocks, wide):
            right = jnp.concatenate(
                [join(disc_ref.at[k, g], range(p0, p0 + wide)) for g in range(groups)], axis=0
            )
            value = dot16(left, right, NN)
            for i in range(wide):
                part = value[:, i * LANES : (i + 1) * LANES]
                square = part * part + SOFTEN
                inverse = lax.rsqrt(square)
                folded = folded + (part + square * inverse)
                slope = column + column * (part * inverse)
                slope_ref[p0 + i] = slope.astype(jnp.bfloat16)
        summed = dot_full(jnp.ones((8, LANES), jnp.float32), folded, NT)
        expo_ref[k : k + 1, :] = summed[0:1] * (0.5 * scale)
        slope_all = join(slope_ref, range(pblocks))
        for g in range(groups):
            for c0 in range(0, cblocks, wide):
                right = jnp.concatenate(
                    [disc_ref[k, g, p, c0 * LANES : (c0 + wide) * LANES, :] for p in range(pblocks)],
                    axis=1,
                )
                back = dot16(slope_all, right, NT)
                for i in range(wide):
                    cash = tables[g][c0 + i].astype(jnp.float32)
                    pull = jnp.sum(back[:, i * LANES : (i + 1) * LANES] * cash, axis=0)
                    cols = slice((c0 + i) * LANES, (c0 + i + 1) * LANES)
                    pull_ref[g : g + 1, cols] = pull[None]
        sens_ref[k] = dot_full(pull_ref[...], scaled_ref[k], NN)
    for g in range(groups):
        rows = slice(g * stations, (g + 1) * stations)
        for k in range(slots):
            part = expo_ref[k : k + 1, g * share : (g + 1) * share]
            out_ref[rows, 0, k * share : (k + 1) * share] = jnp.broadcast_to(
                part, (stations, share)
            )
            line = jnp.zeros((1, nodes), jnp.float32)
            for m in range(groups):
                line = line + route_ref[g * groups + m, 0:1, :nodes] * sens_ref[k, m : m + 1, :]
            begin = slots * share + k * nodes
            out_ref[rows, 0, begin : begin + nodes] = jnp.broadcast_to(line, (stations, nodes))


def price(column, scaled, route, disc, tables, stations, total_paths):
    slots, groups, pblocks = disc.shape[:3]
    nodes = scaled.shape[2]
    paths = pblocks * LANES
    rows = -(-groups // 8) * 8
    return pl.pallas_call(
        functools.partial(price_kernel, stations, 1.0 / total_paths),
        out_shape=jax.ShapeDtypeStruct(
            (groups * stations, 1, slots * (NSETS // groups + nodes)), jnp.float32
        ),
        in_specs=[VM] * (4 + groups),
        out_specs=VM,
        scratch_shapes=[
            pltpu.VMEM((pblocks, NSETS, LANES), jnp.bfloat16),
            pltpu.VMEM((slots, NSETS), jnp.float32),
            pltpu.VMEM((rows, CFG), jnp.float32),
            pltpu.VMEM((slots, rows, nodes), jnp.float32),
        ],
        cost_estimate=pl.CostEstimate(
            flops=4 * slots * groups * CFG * paths * NSETS,
            bytes_accessed=2 * slots * groups * CFG * paths,
            transcendentals=slots * NSETS * paths,
        ),
        compiler_params=pltpu.CompilerParams(
            vmem_limit_bytes=grant(10 * 2**20, 2 * slots * groups * CFG * paths)
        ),
        name="price",
    )(column, scaled, route, disc, *tables)


def collect_kernel(groups, slots, nodes, pick_ref, got_ref, expo_ref, sens_ref):
    stations = got_ref.shape[0] // groups
    dates, share = expo_ref.shape
    expo = jnp.zeros((dates, share), jnp.float32)
    sens = jnp.zeros((dates, nodes), jnp.float32)
    for p in range(stations):
        line = got_ref[p]
        for g in range(1, groups):
            line = line + got_ref[g * stations + p]
        for k in range(slots):
            pick = pick_ref[p * slots + k]
            begin = slots * share + k * nodes
            mine = pick[:, :share] if share <= LANES else pick[:, :1]
            expo = expo + mine * line[:, k * share : (k + 1) * share]
            sens = sens + pick[:, :nodes] * line[:, begin : begin + nodes]
    expo_ref[...] = expo
    sens_ref[...] = sens


def collect(pick, got, groups, slots, nodes):
    dates = pick.shape[1]
    return pl.pallas_call(
        functools.partial(collect_kernel, groups, slots, nodes),
        out_shape=(
            jax.ShapeDtypeStruct((dates, NSETS // groups), jnp.float32),
            jax.ShapeDtypeStruct((dates, nodes), jnp.float32),
        ),
        in_specs=[VM, VM],
        out_specs=(VM, VM),
        compiler_params=pltpu.CompilerParams(vmem_limit_bytes=6 * 2**20),
        name="collect",
    )(pick, got)


def local(curve_store, cash_index, cash_amount, trade_set, date_slot, default_weight):
    groups = lax.axis_size("ccy")
    stations = lax.axis_size("path")
    _, slots, nodes, total_paths = curve_store.shape

    def swap(array, mask):
        return lax.ppermute(array, "ccy", [(i, i ^ mask) for i in range(groups)])

    flows, left, scaled, column, pick, route, *pieces = prepare(
        date_slot, jnp.swapaxes(cash_index[0], 0, 1), jnp.swapaxes(cash_amount[0], 0, 1),
        trade_set, curve_store[0], default_weight, groups, stations,
    )
    others = {m: swap(flows, m) for m in range(2, groups, 2)}
    curves = [pieces[0]] + [swap(pieces[m], m) for m in range(1, groups)]

    tables = {0: build_table(flows)}
    for m in others:
        tables[m] = build_table(others[m])
    for m in list(tables):
        tables[m + 1] = swap(tables[m], 1)
    tables = [tables[m] for m in range(groups)]

    disc = discounts(left, curves)
    payload = price(column, scaled, route, disc, tables, stations, total_paths)
    got = lax.all_to_all(payload, ("ccy", "path"), 0, 0, tiled=True)
    expo, sens = collect(pick, got, groups, slots, nodes)
    return expo, sens[None]


def solution(mesh):
    in_specs = (
        P("ccy", "path", None, None),
        P("ccy", None, None),
        P("ccy", None, None),
        P("ccy", None),
        P(),
        P(),
    )
    out_specs = (P(None, "ccy"), P("ccy", None, None))
    return jax.shard_map(local, mesh=mesh, in_specs=in_specs, out_specs=out_specs, check_vma=False)
```

```python
import functools
import math

import jax
import jax.numpy as jnp
from jax import lax
from jax.experimental import pallas as pl
from jax.experimental.pallas import tpu as pltpu
from jax.sharding import PartitionSpec as P


CFG = 1024
NSETS = 512
SOFTEN = 0.04
HORIZON = 32.0
LOG2E = math.log2(math.e)
LANES = 128
SUB = 16
WIDE = 256

NT = (((1,), (1,)), ((), ()))
NN = (((1,), (0,)), ((), ()))
TN = (((0,), (0,)), ((), ()))
VM = pl.BlockSpec(memory_space=pltpu.VMEM)


def dot16(a, b, dims):
    return lax.dot_general(a, b, dims, preferred_element_type=jnp.float32)


def dot_full(a, b, dims):
    return lax.dot_general(
        a, b, dims, precision=lax.Precision.HIGHEST, preferred_element_type=jnp.float32
    )


def join(ref, blocks):
    return jnp.concatenate([ref[b] for b in blocks], axis=1)


def table_kernel(flow_ref, out_ref, date_t, high_t, one_hot, slot_a, slot_b, acc_ref):
    ncf, trades = flow_ref.shape[0] // 2, flow_ref.shape[1]
    blocks = trades // LANES
    row_ids = lax.broadcasted_iota(jnp.int32, (NSETS // SUB, SUB, LANES), 0) * SUB
    row_ids = (row_ids + lax.broadcasted_iota(jnp.int32, row_ids.shape, 1)).astype(jnp.int16)
    unit = jnp.ones((NSETS // SUB, SUB, LANES), jnp.bfloat16)

    def spread(row):
        return jnp.broadcast_to(row, (SUB, LANES))

    def prepare(b, carry):
        cols = pl.ds(pl.multiple_of(b * LANES, LANES), LANES)
        code = flow_ref[:ncf, cols].astype(jnp.int32)
        total = flow_ref[ncf:, cols]
        date = code & (CFG - 1)
        sets = lax.shift_right_logical(code[0:1, :], CFG.bit_length() - 1)
        for k in range(ncf):
            rows = slice(k * SUB, (k + 1) * SUB)
            date_t[b, rows, :] = spread(date[k : k + 1, :]).astype(jnp.int16)
            high_t[b, rows, :] = spread(total[k : k + 1, :]).astype(jnp.bfloat16)
        mine = spread(sets).astype(jnp.int16)[None]
        chosen = jnp.where(row_ids == mine, unit, jnp.zeros_like(unit))
        one_hot[b] = chosen.reshape(NSETS, LANES)
        return carry

    lax.fori_loop(0, blocks, prepare, 0)

    chunk, tiles = 8, 8
    step = tiles * SUB
    parts = CFG // WIDE
    base = lax.broadcasted_iota(jnp.int32, (tiles, SUB, LANES), 0) * SUB
    base = base + lax.broadcasted_iota(jnp.int32, (tiles, SUB, LANES), 1)
    slots = (slot_a, slot_b)

    def fill(slot, part, b):
        for r in range(0, WIDE, step):
            want = (base + (part * WIDE + r)).astype(jnp.int16)
            acc = jnp.zeros((tiles, SUB, LANES), jnp.bfloat16)
            for k in range(ncf):
                rows = slice(k * SUB, (k + 1) * SUB)
                acc = jnp.where(want == date_t[b, rows, :][None], high_t[b, rows, :][None], acc)
            slot[b, r : r + step, :] = acc.reshape(step, LANES)

    for part in range(parts + 1):
        target, source = slots[part % 2], slots[(part + 1) % 2]
        if part > 0:
            acc_ref[...] = jnp.zeros_like(acc_ref)

        def body(q, carry, part=part, target=target, source=source):
            mine = [q * chunk + i for i in range(chunk)]
            if part > 0:
                acc_ref[...] += dot16(join(one_hot, mine), join(source, mine), NT)
            if part < parts:
                for b in mine:
                    fill(target, part, b)
            return carry

        lax.fori_loop(0, blocks // chunk, body, 0)
        if part > 0:
            block = acc_ref[...].astype(jnp.bfloat16)
            for i in range(WIDE // LANES):
                place = (part - 1) * (WIDE // LANES) + i
                out_ref[place] = block[:, i * LANES : (i + 1) * LANES]


def build_table(flows):
    ncf, trades = flows.shape[0] // 2, flows.shape[1]
    blocks = trades // LANES
    return pl.pallas_call(
        table_kernel,
        out_shape=jax.ShapeDtypeStruct((CFG // LANES, NSETS, LANES), jnp.bfloat16),
        in_specs=[VM],
        out_specs=VM,
        scratch_shapes=[
            pltpu.VMEM((blocks, ncf * SUB, LANES), jnp.int16),
            pltpu.VMEM((blocks, ncf * SUB, LANES), jnp.bfloat16),
            pltpu.VMEM((blocks, NSETS, LANES), jnp.bfloat16),
            pltpu.VMEM((blocks, WIDE, LANES), jnp.bfloat16),
            pltpu.VMEM((blocks, WIDE, LANES), jnp.bfloat16),
            pltpu.VMEM((NSETS, WIDE), jnp.float32),
        ],
        cost_estimate=pl.CostEstimate(
            flops=4 * trades * NSETS * CFG, bytes_accessed=2**21, transcendentals=0
        ),
        compiler_params=pltpu.CompilerParams(vmem_limit_bytes=12 * 2**20),
    )(flows)


def prepare_kernel(groups, stations, scale, *refs):
    sources, outs, scratch = refs[:6], refs[6 : 11 + groups], refs[11 + groups :]
    flow_ref, left_ref, column_ref, pick_ref, route_ref, *pieces = outs
    copies = [
        pltpu.make_async_copy(source, held, scratch[6].at[i])
        for i, (source, held) in enumerate(zip(sources, scratch[:6]))
    ]
    for copy in copies:
        copy.start()
    for copy in copies:
        copy.wait()
    index_ref, amount_ref, set_ref, curve_ref, weight_ref, slot_ref = scratch[:6]
    ncf = index_ref.shape[0]
    slots, nodes, total_paths = curve_ref.shape
    paths = total_paths // groups
    dates = slot_ref.shape[0]
    station, member = lax.axis_index("path"), lax.axis_index("ccy")
    date = index_ref[...]
    flow_ref[:ncf, :] = (date + CFG * set_ref[...]).astype(jnp.float32)
    total = jnp.zeros(date.shape, jnp.float32)
    for k in range(ncf):
        same = date == index_ref[k : k + 1, :]
        total = total + jnp.where(same, amount_ref[k : k + 1, :], 0.0)
    flow_ref[ncf:, :] = total
    for mask, piece in enumerate(pieces):
        begin = pl.multiple_of((member ^ mask) * paths, LANES)
        for k in range(slots):
            piece[k] = curve_ref[k, :, pl.ds(begin, paths)]
    lead = (lax.broadcasted_iota(jnp.int32, (8, LANES), 0) == 0).astype(jnp.float32)
    starts = []
    for k in range(slots):
        date, found = 0, 0
        for d in range(dates):
            hit = slot_ref[d] == station * slots + k
            date = jnp.where(hit, d, date)
            found = jnp.where(hit, 1, found)
        row = weight_ref[pl.ds(date, 1), :] * (0.5 * scale) * found.astype(jnp.float32)
        column_ref[k] = dot_full(jnp.broadcast_to(row, (8, NSETS)), lead, TN)
        starts.append(0.5 * (date.astype(jnp.float32) + 1.0))
    lane = lax.broadcasted_iota(jnp.int32, (CFG, slots * nodes), 1)
    start = jnp.zeros((CFG, slots * nodes), jnp.float32)
    for k in range(slots):
        start = jnp.where(lane >= k * nodes, starts[k], start)
    grid = lax.broadcasted_iota(jnp.int32, (CFG, slots * nodes), 0).astype(jnp.float32)
    remain = HORIZON * (grid + 1.0) / CFG - start
    node = (lane & (nodes - 1)).astype(jnp.float32)
    tenor = HORIZON * (node + 1.0) / nodes
    clipped = jnp.clip(remain, HORIZON / nodes, HORIZON)
    weight = jnp.maximum(0.0, 1.0 - jnp.abs(clipped - tenor) * (nodes / HORIZON))
    scaled = weight * (remain * (-LOG2E))
    high = scaled.astype(jnp.bfloat16)
    rest = scaled - high.astype(jnp.float32)
    mid = rest.astype(jnp.bfloat16)
    low = (rest - mid.astype(jnp.float32)).astype(jnp.bfloat16)
    dead = jnp.where((node == 0.0) & (remain <= 0.0), -1e30, 0.0).astype(jnp.bfloat16)
    for k in range(slots):
        own = slice(k * nodes, (k + 1) * nodes)
        left = jnp.concatenate([part[:, own] for part in (high, mid, low, dead)], axis=1)
        for i in range(4 * nodes // LANES):
            left_ref[k, i] = left[:, i * LANES : (i + 1) * LANES]
    line = lax.broadcasted_iota(jnp.int32, (dates, LANES), 0)
    slot_of = jnp.zeros((dates, LANES), jnp.int32)
    for d in range(dates):
        slot_of = jnp.where(line == d, slot_ref[d], slot_of)
    for i in range(stations * slots):
        pick_ref[i] = (slot_of == i).astype(jnp.float32)
    for g in range(groups):
        for m in range(groups):
            chosen = ((member ^ g) == m).astype(jnp.float32)
            route_ref[g * groups + m] = jnp.full((8, LANES), chosen, jnp.float32)


def prepare(date_slot, index, amount, sets, curve, weights, groups, stations):
    ncf, trades = index.shape
    slots, nodes, total_paths = curve.shape
    dates = date_slot.shape[0]
    sources = (index, amount, sets, curve, weights, date_slot)
    return pl.pallas_call(
        functools.partial(prepare_kernel, groups, stations, 1.0 / total_paths),
        out_shape=(
            jax.ShapeDtypeStruct((2 * ncf, trades), jnp.float32),
            jax.ShapeDtypeStruct((slots, 4 * nodes // LANES, CFG, LANES), jnp.bfloat16),
            jax.ShapeDtypeStruct((slots, NSETS, LANES), jnp.float32),
            jax.ShapeDtypeStruct((stations * slots, dates, LANES), jnp.float32),
            jax.ShapeDtypeStruct((groups * groups, 8, LANES), jnp.float32),
        )
        + (jax.ShapeDtypeStruct((slots, nodes, total_paths // groups), jnp.bfloat16),) * groups,
        in_specs=[pl.BlockSpec(memory_space=pltpu.HBM)] * 6,
        out_specs=(VM,) * (5 + groups),
        scratch_shapes=[pltpu.VMEM(source.shape, source.dtype) for source in sources[:5]]
        + [pltpu.SMEM((dates,), jnp.int32), pltpu.SemaphoreType.DMA((6,))],
        cost_estimate=pl.CostEstimate(flops=2**22, bytes_accessed=2**21, transcendentals=0),
        compiler_params=pltpu.CompilerParams(
            vmem_limit_bytes=14 * 2**20 + 6 * slots * nodes * total_paths
        ),
        name="prepare",
    )(*[pltpu.with_memory_space_constraint(source, pltpu.HBM) for source in sources])


def grant(own, shared):
    return own if shared <= 2**24 else 62 * 2**20


def disc_kernel(groups, left_ref, *refs):
    curves, (disc_ref, rhs) = refs[:groups], refs[groups:]
    slots, nodes, paths = curves[0].shape
    depth = rhs.shape[0]
    rhs[3 * nodes :, :] = jnp.ones((depth - 3 * nodes, paths), jnp.bfloat16)
    for k in range(slots):
        left = join(left_ref.at[k], range(depth // LANES))
        for g in range(groups):
            for copy in range(3):
                rhs[copy * nodes : (copy + 1) * nodes, :] = curves[g][k]
            for p0 in range(0, paths, WIDE):
                block = jnp.exp2(dot16(left, rhs[:, p0 : p0 + WIDE], NN)).astype(jnp.bfloat16)
                for i in range(WIDE // LANES):
                    disc_ref[k, g, p0 // LANES + i] = block[:, i * LANES : (i + 1) * LANES]


def discounts(left, curves):
    slots, nodes, paths = curves[0].shape
    groups = len(curves)
    return pl.pallas_call(
        functools.partial(disc_kernel, groups),
        out_shape=jax.ShapeDtypeStruct(
            (slots, groups, paths // LANES, CFG, LANES), jnp.bfloat16
        ),
        in_specs=[VM] * (1 + groups),
        out_specs=VM,
        scratch_shapes=[pltpu.VMEM((4 * nodes, paths), jnp.bfloat16)],
        cost_estimate=pl.CostEstimate(
            flops=2 * slots * groups * CFG * paths * 4 * nodes,
            bytes_accessed=2 * slots * groups * CFG * paths,
            transcendentals=slots * groups * CFG * paths,
        ),
        compiler_params=pltpu.CompilerParams(
            vmem_limit_bytes=grant(6 * 2**20, 2 * slots * groups * CFG * paths)
        ),
        name="discounts",
    )(left, *curves)


def price_kernel(stations, scale, column_ref, left_ref, route_ref, disc_ref, *refs):
    groups = disc_ref.shape[1]
    tables = refs[:groups]
    out_ref, value_ref, slope_ref, expo_ref, pull_ref, sens_ref = refs[groups:]
    slots = disc_ref.shape[0]
    pblocks = disc_ref.shape[2]
    cblocks = CFG // LANES
    nodes = sens_ref.shape[2]
    share = NSETS // groups
    wide = WIDE // LANES
    pull_ref[...] = jnp.zeros_like(pull_ref)

    def values(k, p0):
        left = jnp.concatenate([join(tables[g], range(cblocks)) for g in range(groups)], axis=1)
        right = jnp.concatenate(
            [join(disc_ref.at[k, g], range(p0, p0 + wide)) for g in range(groups)], axis=0
        )
        value = dot16(left, right, NN)
        for i in range(wide):
            value_ref[k, p0 + i] = value[:, i * LANES : (i + 1) * LANES]

    def slopes(k):
        column = column_ref[k]
        folded = jnp.zeros((NSETS, LANES), jnp.float32)
        for p in range(pblocks):
            part = value_ref[k, p]
            square = part * part + SOFTEN
            inverse = lax.rsqrt(square)
            folded = folded + (part + square * inverse)
            slope = column + column * (part * inverse)
            slope_ref[k, p] = slope.astype(jnp.bfloat16)
        summed = dot_full(jnp.ones((8, LANES), jnp.float32), folded, NT)
        expo_ref[k : k + 1, :] = summed[0:1] * (0.5 * scale)

    def pulls(k, g):
        slope_all = join(slope_ref.at[k], range(pblocks))
        for c0 in range(0, cblocks, wide):
            right = jnp.concatenate(
                [disc_ref[k, g, p, c0 * LANES : (c0 + wide) * LANES, :] for p in range(pblocks)],
                axis=1,
            )
            back = dot16(slope_all, right, NT)
            for i in range(wide):
                cash = tables[g][c0 + i].astype(jnp.float32)
                pull = jnp.sum(back[:, i * LANES : (i + 1) * LANES] * cash, axis=0)
                cols = slice((c0 + i) * LANES, (c0 + i + 1) * LANES)
                pull_ref[k, g : g + 1, cols] = pull[None]

    for p0 in range(0, pblocks, wide):
        values(0, p0)
    for k in range(slots):
        beside = []
        if k + 1 < slots:
            beside = [functools.partial(values, k + 1, p0) for p0 in range(0, pblocks, wide)]
        elif k > 0:
            beside = [functools.partial(pulls, k - 1, g) for g in range(groups)]
        for work in beside[:1]:
            work()
        slopes(k)
        for work in beside[1:]:
            work()
    for k in [*range(slots - 2), slots - 1]:
        for g in range(groups):
            pulls(k, g)
    for k in range(slots):
        pull = pull_ref[k]
        terms = []
        for _ in range(3):
            term = pull.astype(jnp.bfloat16)
            pull = pull - term.astype(jnp.float32)
            terms.append(term.astype(jnp.float32))
        rows = jnp.concatenate(terms, axis=0).astype(jnp.bfloat16)
        crossed = dot16(rows, join(left_ref.at[k], range(left_ref.shape[1])), NN)
        count = pull_ref.shape[1]
        sens = jnp.zeros((count, nodes), jnp.float32)
        for i in range(3):
            for j in range(3):
                sens = sens + crossed[i * count : (i + 1) * count, j * nodes : (j + 1) * nodes]
        sens_ref[k] = sens * (1.0 / LOG2E)
    for g in range(groups):
        rows = slice(g * stations, (g + 1) * stations)
        for k in range(slots):
            part = expo_ref[k : k + 1, g * share : (g + 1) * share]
            out_ref[rows, 0, k * share : (k + 1) * share] = jnp.broadcast_to(
                part, (stations, share)
            )
            line = jnp.zeros((1, nodes), jnp.float32)
            for m in range(groups):
                line = line + route_ref[g * groups + m, 0:1, :nodes] * sens_ref[k, m : m + 1, :]
            begin = slots * share + k * nodes
            out_ref[rows, 0, begin : begin + nodes] = jnp.broadcast_to(line, (stations, nodes))


def price(column, left, route, disc, tables, stations, total_paths):
    slots, groups, pblocks = disc.shape[:3]
    nodes = left.shape[1] * LANES // 4
    paths = pblocks * LANES
    rows = -(-groups // 8) * 8
    return pl.pallas_call(
        functools.partial(price_kernel, stations, 1.0 / total_paths),
        out_shape=jax.ShapeDtypeStruct(
            (groups * stations, 1, slots * (NSETS // groups + nodes)), jnp.float32
        ),
        in_specs=[VM] * (4 + groups),
        out_specs=VM,
        scratch_shapes=[
            pltpu.VMEM((slots, pblocks, NSETS, LANES), jnp.float32),
            pltpu.VMEM((slots, pblocks, NSETS, LANES), jnp.bfloat16),
            pltpu.VMEM((slots, NSETS), jnp.float32),
            pltpu.VMEM((slots, rows, CFG), jnp.float32),
            pltpu.VMEM((slots, rows, nodes), jnp.float32),
        ],
        cost_estimate=pl.CostEstimate(
            flops=4 * slots * groups * CFG * paths * NSETS,
            bytes_accessed=2 * slots * groups * CFG * paths,
            transcendentals=slots * NSETS * paths,
        ),
        compiler_params=pltpu.CompilerParams(
            vmem_limit_bytes=grant(10 * 2**20, 2 * slots * groups * CFG * paths)
        ),
        name="price",
    )(column, left, route, disc, *tables)


def collect_kernel(groups, slots, nodes, pick_ref, got_ref, expo_ref, sens_ref):
    stations = got_ref.shape[0] // groups
    dates, share = expo_ref.shape
    expo = jnp.zeros((dates, share), jnp.float32)
    sens = jnp.zeros((dates, nodes), jnp.float32)
    for p in range(stations):
        line = got_ref[p]
        for g in range(1, groups):
            line = line + got_ref[g * stations + p]
        for k in range(slots):
            pick = pick_ref[p * slots + k]
            begin = slots * share + k * nodes
            mine = pick[:, :share] if share <= LANES else pick[:, :1]
            expo = expo + mine * line[:, k * share : (k + 1) * share]
            sens = sens + pick[:, :nodes] * line[:, begin : begin + nodes]
    expo_ref[...] = expo
    sens_ref[...] = sens


def collect(pick, got, groups, slots, nodes):
    dates = pick.shape[1]
    return pl.pallas_call(
        functools.partial(collect_kernel, groups, slots, nodes),
        out_shape=(
            jax.ShapeDtypeStruct((dates, NSETS // groups), jnp.float32),
            jax.ShapeDtypeStruct((dates, nodes), jnp.float32),
        ),
        in_specs=[VM, VM],
        out_specs=(VM, VM),
        compiler_params=pltpu.CompilerParams(vmem_limit_bytes=6 * 2**20),
        name="collect",
    )(pick, got)


def local(curve_store, cash_index, cash_amount, trade_set, date_slot, default_weight):
    groups = lax.axis_size("ccy")
    stations = lax.axis_size("path")
    _, slots, nodes, total_paths = curve_store.shape

    def swap(array, mask):
        return lax.ppermute(array, "ccy", [(i, i ^ mask) for i in range(groups)])

    flows, left, column, pick, route, *pieces = prepare(
        date_slot, jnp.swapaxes(cash_index[0], 0, 1), jnp.swapaxes(cash_amount[0], 0, 1),
        trade_set, curve_store[0], default_weight, groups, stations,
    )
    others = {m: swap(flows, m) for m in range(2, groups, 2)}
    curves = [pieces[0]] + [swap(pieces[m], m) for m in range(1, groups)]

    tables = {0: build_table(flows)}
    for m in others:
        tables[m] = build_table(others[m])
    for m in list(tables):
        tables[m + 1] = swap(tables[m], 1)
    tables = [tables[m] for m in range(groups)]

    disc = discounts(left, curves)
    payload = price(column, left, route, disc, tables, stations, total_paths)
    got = lax.all_to_all(payload, ("ccy", "path"), 0, 0, tiled=True)
    expo, sens = collect(pick, got, groups, slots, nodes)
    return expo, sens[None]


def solution(mesh):
    in_specs = (
        P("ccy", "path", None, None),
        P("ccy", None, None),
        P("ccy", None, None),
        P("ccy", None),
        P(),
        P(),
    )
    out_specs = (P(None, "ccy"), P("ccy", None, None))
    return jax.shard_map(local, mesh=mesh, in_specs=in_specs, out_specs=out_specs, check_vma=False)
```

```python
import functools
import math

import jax
import jax.numpy as jnp
from jax import lax
from jax.experimental import pallas as pl
from jax.experimental.pallas import tpu as pltpu
from jax.sharding import PartitionSpec as P


CFG = 1024
NSETS = 512
SOFTEN = 0.04
HORIZON = 32.0
LOG2E = math.log2(math.e)
LANES = 128
SUB = 16
WIDE = 256

NT = (((1,), (1,)), ((), ()))
NN = (((1,), (0,)), ((), ()))
TN = (((0,), (0,)), ((), ()))
VM = pl.BlockSpec(memory_space=pltpu.VMEM)


def dot16(a, b, dims):
    return lax.dot_general(a, b, dims, preferred_element_type=jnp.float32)


def dot_full(a, b, dims):
    return lax.dot_general(
        a, b, dims, precision=lax.Precision.HIGHEST, preferred_element_type=jnp.float32
    )


def join(ref, blocks):
    return jnp.concatenate([ref[b] for b in blocks], axis=1)


def table_kernel(flow_ref, out_ref, date_t, high_t, one_hot, slot_a, slot_b):
    ncf, trades = flow_ref.shape[0] // 2, flow_ref.shape[1]
    blocks = trades // LANES
    row_ids = lax.broadcasted_iota(jnp.int32, (NSETS // SUB, SUB, LANES), 0) * SUB
    row_ids = (row_ids + lax.broadcasted_iota(jnp.int32, row_ids.shape, 1)).astype(jnp.int16)
    unit = jnp.ones((NSETS // SUB, SUB, LANES), jnp.bfloat16)

    def spread(row):
        return jnp.broadcast_to(row, (SUB, LANES))

    def prepare(b, carry):
        cols = pl.ds(pl.multiple_of(b * LANES, LANES), LANES)
        code = flow_ref[:ncf, cols].astype(jnp.int32)
        total = flow_ref[ncf:, cols]
        date = code & (CFG - 1)
        sets = lax.shift_right_logical(code[0:1, :], CFG.bit_length() - 1)
        for k in range(ncf):
            rows = slice(k * SUB, (k + 1) * SUB)
            date_t[b, rows, :] = spread(date[k : k + 1, :]).astype(jnp.int16)
            high_t[b, rows, :] = spread(total[k : k + 1, :]).astype(jnp.bfloat16)
        mine = spread(sets).astype(jnp.int16)[None]
        chosen = jnp.where(row_ids == mine, unit, jnp.zeros_like(unit))
        one_hot[b] = chosen.reshape(NSETS, LANES)
        return carry

    lax.fori_loop(0, blocks, prepare, 0)

    tiles = 8
    step = tiles * SUB
    parts = CFG // WIDE
    chunk = blocks // 2
    base = lax.broadcasted_iota(jnp.int32, (tiles, SUB, LANES), 0) * SUB
    base = base + lax.broadcasted_iota(jnp.int32, (tiles, SUB, LANES), 1)
    slots = (slot_a, slot_b)

    def fill(slot, part, b):
        for r in range(0, WIDE, step):
            want = (base + (part * WIDE + r)).astype(jnp.int16)
            acc = jnp.zeros((tiles, SUB, LANES), jnp.bfloat16)
            for k in range(ncf):
                rows = slice(k * SUB, (k + 1) * SUB)
                acc = jnp.where(want == date_t[b, rows, :][None], high_t[b, rows, :][None], acc)
            slot[b, r : r + step, :] = acc.reshape(step, LANES)

    def multiply(slot, part, rows):
        left = jnp.concatenate([one_hot[b, rows, :] for b in range(blocks)], axis=1)
        block = dot16(left, join(slot, range(blocks)), NT).astype(jnp.bfloat16)
        for i in range(WIDE // LANES):
            place = part * (WIDE // LANES) + i
            out_ref[place, rows, :] = block[:, i * LANES : (i + 1) * LANES]

    for part in range(parts):
        target, source = slots[part % 2], slots[(part + 1) % 2]

        def body(q, carry, part=part, target=target, source=source):
            if part > 0:
                half = pl.ds(pl.multiple_of(q * (NSETS // 2), NSETS // 2), NSETS // 2)
                multiply(source, part - 1, half)
            for i in range(chunk):
                fill(target, part, q * chunk + i)
            return carry

        lax.fori_loop(0, 2, body, 0)
    multiply(slots[(parts + 1) % 2], parts - 1, slice(0, NSETS))


def build_table(flows):
    ncf, trades = flows.shape[0] // 2, flows.shape[1]
    blocks = trades // LANES
    return pl.pallas_call(
        table_kernel,
        out_shape=jax.ShapeDtypeStruct((CFG // LANES, NSETS, LANES), jnp.bfloat16),
        in_specs=[VM],
        out_specs=VM,
        scratch_shapes=[
            pltpu.VMEM((blocks, ncf * SUB, LANES), jnp.int16),
            pltpu.VMEM((blocks, ncf * SUB, LANES), jnp.bfloat16),
            pltpu.VMEM((blocks, NSETS, LANES), jnp.bfloat16),
            pltpu.VMEM((blocks, WIDE, LANES), jnp.bfloat16),
            pltpu.VMEM((blocks, WIDE, LANES), jnp.bfloat16),
        ],
        cost_estimate=pl.CostEstimate(
            flops=4 * trades * NSETS * CFG, bytes_accessed=2**21, transcendentals=0
        ),
        compiler_params=pltpu.CompilerParams(vmem_limit_bytes=12 * 2**20),
    )(flows)


def prepare_kernel(groups, stations, scale, *refs):
    sources, outs, scratch = refs[:6], refs[6 : 11 + groups], refs[11 + groups :]
    flow_ref, left_ref, column_ref, pick_ref, route_ref, *pieces = outs
    copies = [
        pltpu.make_async_copy(source, held, scratch[6].at[i])
        for i, (source, held) in enumerate(zip(sources, scratch[:6]))
    ]
    for copy in copies:
        copy.start()
    index_ref, amount_ref, set_ref, curve_ref, weight_ref, slot_ref = scratch[:6]
    ncf = index_ref.shape[0]
    slots, nodes, total_paths = curve_ref.shape
    paths = total_paths // groups
    dates = slot_ref.shape[0]
    station, member = lax.axis_index("path"), lax.axis_index("ccy")
    copies[5].wait()
    starts, lines = [], []
    for k in range(slots):
        date, found = 0, 0
        for d in range(dates):
            hit = slot_ref[d] == station * slots + k
            date = jnp.where(hit, d, date)
            found = jnp.where(hit, 1, found)
        starts.append(0.5 * (date.astype(jnp.float32) + 1.0))
        lines.append((date, found))
    lane = lax.broadcasted_iota(jnp.int32, (CFG, slots * nodes), 1)
    start = jnp.zeros((CFG, slots * nodes), jnp.float32)
    for k in range(slots):
        start = jnp.where(lane >= k * nodes, starts[k], start)
    grid = lax.broadcasted_iota(jnp.int32, (CFG, slots * nodes), 0).astype(jnp.float32)
    remain = HORIZON * (grid + 1.0) / CFG - start
    node = (lane & (nodes - 1)).astype(jnp.float32)
    tenor = HORIZON * (node + 1.0) / nodes
    clipped = jnp.clip(remain, HORIZON / nodes, HORIZON)
    weight = jnp.maximum(0.0, 1.0 - jnp.abs(clipped - tenor) * (nodes / HORIZON))
    scaled = weight * (remain * (-LOG2E))
    high = scaled.astype(jnp.bfloat16)
    rest = scaled - high.astype(jnp.float32)
    mid = rest.astype(jnp.bfloat16)
    low = (rest - mid.astype(jnp.float32)).astype(jnp.bfloat16)
    dead = jnp.where((node == 0.0) & (remain <= 0.0), -1e30, 0.0).astype(jnp.bfloat16)
    for k in range(slots):
        own = slice(k * nodes, (k + 1) * nodes)
        left = jnp.concatenate([part[:, own] for part in (high, mid, low, dead)], axis=1)
        for i in range(4 * nodes // LANES):
            left_ref[k, i] = left[:, i * LANES : (i + 1) * LANES]
    line = lax.broadcasted_iota(jnp.int32, (dates, LANES), 0)
    slot_of = jnp.zeros((dates, LANES), jnp.int32)
    for d in range(dates):
        slot_of = jnp.where(line == d, slot_ref[d], slot_of)
    for i in range(stations * slots):
        pick_ref[i] = (slot_of == i).astype(jnp.float32)
    for g in range(groups):
        for m in range(groups):
            chosen = ((member ^ g) == m).astype(jnp.float32)
            route_ref[g * groups + m] = jnp.full((8, LANES), chosen, jnp.float32)
    for copy in copies[:5]:
        copy.wait()

    def pack(b, carry):
        cols = pl.ds(pl.multiple_of(b * LANES, LANES), LANES)
        date, amount = index_ref[:, cols], amount_ref[:, cols]
        flow_ref[:ncf, cols] = (date + CFG * set_ref[:, cols]).astype(jnp.float32)
        total = jnp.zeros((ncf, LANES), jnp.float32)
        for k in range(ncf):
            same = date == date[k : k + 1, :]
            total = total + jnp.where(same, amount[k : k + 1, :], 0.0)
        flow_ref[ncf:, cols] = total
        return carry

    lax.fori_loop(0, index_ref.shape[1] // LANES, pack, 0)
    for mask, piece in enumerate(pieces):
        begin = pl.multiple_of((member ^ mask) * paths, LANES)
        for k in range(slots):
            piece[k] = curve_ref[k, :, pl.ds(begin, paths)]
    term = lax.broadcasted_iota(jnp.int32, (SUB, NSETS), 0)
    for k, (date, found) in enumerate(lines):
        row = weight_ref[pl.ds(date, 1), :] * (0.5 * scale) * found.astype(jnp.float32)
        rest = jnp.broadcast_to(row, (SUB, NSETS))
        terms = jnp.zeros((SUB, NSETS), jnp.float32)
        for i in range(3):
            part = rest.astype(jnp.bfloat16).astype(jnp.float32)
            terms = jnp.where(term == i, part, terms)
            rest = rest - part
        column_ref[k] = dot16(
            terms.astype(jnp.bfloat16), jnp.ones((SUB, LANES), jnp.bfloat16), TN
        )


def prepare(date_slot, index, amount, sets, curve, weights, groups, stations):
    ncf, trades = index.shape
    slots, nodes, total_paths = curve.shape
    dates = date_slot.shape[0]
    sources = (index, amount, sets, curve, weights, date_slot)
    return pl.pallas_call(
        functools.partial(prepare_kernel, groups, stations, 1.0 / total_paths),
        out_shape=(
            jax.ShapeDtypeStruct((2 * ncf, trades), jnp.float32),
            jax.ShapeDtypeStruct((slots, 4 * nodes // LANES, CFG, LANES), jnp.bfloat16),
            jax.ShapeDtypeStruct((slots, NSETS, LANES), jnp.float32),
            jax.ShapeDtypeStruct((stations * slots, dates, LANES), jnp.float32),
            jax.ShapeDtypeStruct((groups * groups, 8, LANES), jnp.float32),
        )
        + (jax.ShapeDtypeStruct((slots, nodes, total_paths // groups), jnp.bfloat16),) * groups,
        in_specs=[pl.BlockSpec(memory_space=pltpu.HBM)] * 6,
        out_specs=(VM,) * (5 + groups),
        scratch_shapes=[pltpu.VMEM(source.shape, source.dtype) for source in sources[:5]]
        + [pltpu.SMEM((dates,), jnp.int32), pltpu.SemaphoreType.DMA((6,))],
        cost_estimate=pl.CostEstimate(flops=2**22, bytes_accessed=2**21, transcendentals=0),
        compiler_params=pltpu.CompilerParams(
            vmem_limit_bytes=14 * 2**20 + 6 * slots * nodes * total_paths
        ),
        name="prepare",
    )(*[pltpu.with_memory_space_constraint(source, pltpu.HBM) for source in sources])


def grant(own, shared):
    return own if shared <= 2**24 else 62 * 2**20


def disc_kernel(groups, left_ref, *refs):
    curves, (disc_ref, rhs) = refs[:groups], refs[groups:]
    slots, nodes, paths = curves[0].shape
    depth = rhs.shape[0]
    rhs[3 * nodes :, :] = jnp.ones((depth - 3 * nodes, paths), jnp.bfloat16)
    for k in range(slots):
        left = join(left_ref.at[k], range(depth // LANES))
        for g in range(groups):
            for copy in range(3):
                rhs[copy * nodes : (copy + 1) * nodes, :] = curves[g][k]
            for p0 in range(0, paths, WIDE):
                block = jnp.exp2(dot16(left, rhs[:, p0 : p0 + WIDE], NN)).astype(jnp.bfloat16)
                for i in range(WIDE // LANES):
                    disc_ref[k, g, p0 // LANES + i] = block[:, i * LANES : (i + 1) * LANES]


def discounts(left, curves):
    slots, nodes, paths = curves[0].shape
    groups = len(curves)
    return pl.pallas_call(
        functools.partial(disc_kernel, groups),
        out_shape=jax.ShapeDtypeStruct(
            (slots, groups, paths // LANES, CFG, LANES), jnp.bfloat16
        ),
        in_specs=[VM] * (1 + groups),
        out_specs=VM,
        scratch_shapes=[pltpu.VMEM((4 * nodes, paths), jnp.bfloat16)],
        cost_estimate=pl.CostEstimate(
            flops=2 * slots * groups * CFG * paths * 4 * nodes,
            bytes_accessed=2 * slots * groups * CFG * paths,
            transcendentals=slots * groups * CFG * paths,
        ),
        compiler_params=pltpu.CompilerParams(
            vmem_limit_bytes=grant(6 * 2**20, 2 * slots * groups * CFG * paths)
        ),
        name="discounts",
    )(left, *curves)


def price_kernel(stations, scale, column_ref, left_ref, route_ref, disc_ref, *refs):
    groups = disc_ref.shape[1]
    tables = refs[:groups]
    out_ref, value_ref, slope_ref, expo_ref, pull_ref, sens_ref = refs[groups:]
    slots = disc_ref.shape[0]
    pblocks = disc_ref.shape[2]
    cblocks = CFG // LANES
    nodes = sens_ref.shape[2]
    share = NSETS // groups
    wide = WIDE // LANES
    pull_ref[...] = jnp.zeros_like(pull_ref)

    def values(k, p0):
        left = jnp.concatenate([join(tables[g], range(cblocks)) for g in range(groups)], axis=1)
        right = jnp.concatenate(
            [join(disc_ref.at[k, g], range(p0, p0 + wide)) for g in range(groups)], axis=0
        )
        value = dot16(left, right, NN)
        for i in range(wide):
            value_ref[k, p0 + i] = value[:, i * LANES : (i + 1) * LANES]

    def slopes(k):
        column = column_ref[k]
        folded = jnp.zeros((NSETS, LANES), jnp.float32)
        for p in range(pblocks):
            part = value_ref[k, p]
            square = part * part + SOFTEN
            inverse = lax.rsqrt(square)
            folded = folded + (part + square * inverse)
            slope = column + column * (part * inverse)
            slope_ref[k, p] = slope.astype(jnp.bfloat16)
        summed = dot_full(jnp.ones((8, LANES), jnp.float32), folded, NT)
        expo_ref[k : k + 1, :] = summed[0:1] * (0.5 * scale)

    def pulls(k, g):
        slope_all = join(slope_ref.at[k], range(pblocks))
        for c0 in range(0, cblocks, wide):
            right = jnp.concatenate(
                [disc_ref[k, g, p, c0 * LANES : (c0 + wide) * LANES, :] for p in range(pblocks)],
                axis=1,
            )
            back = dot16(slope_all, right, NT)
            for i in range(wide):
                cash = tables[g][c0 + i].astype(jnp.float32)
                pull = jnp.sum(back[:, i * LANES : (i + 1) * LANES] * cash, axis=0)
                cols = slice((c0 + i) * LANES, (c0 + i + 1) * LANES)
                pull_ref[k, g : g + 1, cols] = pull[None]

    for p0 in range(0, pblocks, wide):
        values(0, p0)
    for k in range(slots):
        beside = []
        if k + 1 < slots:
            beside = [functools.partial(values, k + 1, p0) for p0 in range(0, pblocks, wide)]
        elif k > 0:
            beside = [functools.partial(pulls, k - 1, g) for g in range(groups)]
        for work in beside[:1]:
            work()
        slopes(k)
        for work in beside[1:]:
            work()
    for k in [*range(slots - 2), slots - 1]:
        for g in range(groups):
            pulls(k, g)
    for k in range(slots):
        pull = pull_ref[k]
        terms = []
        for _ in range(3):
            term = pull.astype(jnp.bfloat16)
            pull = pull - term.astype(jnp.float32)
            terms.append(term.astype(jnp.float32))
        rows = jnp.concatenate(terms, axis=0).astype(jnp.bfloat16)
        crossed = dot16(rows, join(left_ref.at[k], range(left_ref.shape[1])), NN)
        count = pull_ref.shape[1]
        sens = jnp.zeros((count, nodes), jnp.float32)
        for i in range(3):
            for j in range(3):
                sens = sens + crossed[i * count : (i + 1) * count, j * nodes : (j + 1) * nodes]
        sens_ref[k] = sens * (1.0 / LOG2E)
    for g in range(groups):
        rows = slice(g * stations, (g + 1) * stations)
        for k in range(slots):
            part = expo_ref[k : k + 1, g * share : (g + 1) * share]
            out_ref[rows, 0, k * share : (k + 1) * share] = jnp.broadcast_to(
                part, (stations, share)
            )
            line = jnp.zeros((1, nodes), jnp.float32)
            for m in range(groups):
                line = line + route_ref[g * groups + m, 0:1, :nodes] * sens_ref[k, m : m + 1, :]
            begin = slots * share + k * nodes
            out_ref[rows, 0, begin : begin + nodes] = jnp.broadcast_to(line, (stations, nodes))


def price(column, left, route, disc, tables, stations, total_paths):
    slots, groups, pblocks = disc.shape[:3]
    nodes = left.shape[1] * LANES // 4
    paths = pblocks * LANES
    rows = -(-groups // 8) * 8
    return pl.pallas_call(
        functools.partial(price_kernel, stations, 1.0 / total_paths),
        out_shape=jax.ShapeDtypeStruct(
            (groups * stations, 1, slots * (NSETS // groups + nodes)), jnp.float32
        ),
        in_specs=[VM] * (4 + groups),
        out_specs=VM,
        scratch_shapes=[
            pltpu.VMEM((slots, pblocks, NSETS, LANES), jnp.float32),
            pltpu.VMEM((slots, pblocks, NSETS, LANES), jnp.bfloat16),
            pltpu.VMEM((slots, NSETS), jnp.float32),
            pltpu.VMEM((slots, rows, CFG), jnp.float32),
            pltpu.VMEM((slots, rows, nodes), jnp.float32),
        ],
        cost_estimate=pl.CostEstimate(
            flops=4 * slots * groups * CFG * paths * NSETS,
            bytes_accessed=2 * slots * groups * CFG * paths,
            transcendentals=slots * NSETS * paths,
        ),
        compiler_params=pltpu.CompilerParams(
            vmem_limit_bytes=grant(10 * 2**20, 2 * slots * groups * CFG * paths)
        ),
        name="price",
    )(column, left, route, disc, *tables)


def collect_kernel(groups, slots, nodes, pick_ref, got_ref, expo_ref, sens_ref):
    stations = got_ref.shape[0] // groups
    dates, share = expo_ref.shape
    expo = jnp.zeros((dates, share), jnp.float32)
    sens = jnp.zeros((dates, nodes), jnp.float32)
    for p in range(stations):
        line = got_ref[p]
        for g in range(1, groups):
            line = line + got_ref[g * stations + p]
        for k in range(slots):
            pick = pick_ref[p * slots + k]
            begin = slots * share + k * nodes
            mine = pick[:, :share] if share <= LANES else pick[:, :1]
            expo = expo + mine * line[:, k * share : (k + 1) * share]
            sens = sens + pick[:, :nodes] * line[:, begin : begin + nodes]
    expo_ref[...] = expo
    sens_ref[...] = sens


def collect(pick, got, groups, slots, nodes):
    dates = pick.shape[1]
    return pl.pallas_call(
        functools.partial(collect_kernel, groups, slots, nodes),
        out_shape=(
            jax.ShapeDtypeStruct((dates, NSETS // groups), jnp.float32),
            jax.ShapeDtypeStruct((dates, nodes), jnp.float32),
        ),
        in_specs=[VM, VM],
        out_specs=(VM, VM),
        compiler_params=pltpu.CompilerParams(vmem_limit_bytes=6 * 2**20),
        name="collect",
    )(pick, got)


def local(curve_store, cash_index, cash_amount, trade_set, date_slot, default_weight):
    groups = lax.axis_size("ccy")
    stations = lax.axis_size("path")
    _, slots, nodes, total_paths = curve_store.shape

    def swap(array, mask):
        return lax.ppermute(array, "ccy", [(i, i ^ mask) for i in range(groups)])

    flows, left, column, pick, route, *pieces = prepare(
        date_slot, jnp.swapaxes(cash_index[0], 0, 1), jnp.swapaxes(cash_amount[0], 0, 1),
        trade_set, curve_store[0], default_weight, groups, stations,
    )
    others = {m: swap(flows, m) for m in range(2, groups, 2)}
    curves = [pieces[0]] + [swap(pieces[m], m) for m in range(1, groups)]

    tables = {0: build_table(flows)}
    for m in others:
        tables[m] = build_table(others[m])
    for m in list(tables):
        tables[m + 1] = swap(tables[m], 1)
    tables = [tables[m] for m in range(groups)]

    disc = discounts(left, curves)
    payload = price(column, left, route, disc, tables, stations, total_paths)
    got = lax.all_to_all(payload, ("ccy", "path"), 0, 0, tiled=True)
    expo, sens = collect(pick, got, groups, slots, nodes)
    return expo, sens[None]


def solution(mesh):
    in_specs = (
        P("ccy", "path", None, None),
        P("ccy", None, None),
        P("ccy", None, None),
        P("ccy", None),
        P(),
        P(),
    )
    out_specs = (P(None, "ccy"), P("ccy", None, None))
    return jax.shard_map(local, mesh=mesh, in_specs=in_specs, out_specs=out_specs, check_vma=False)
```

```python
import functools
import math

import jax
import jax.numpy as jnp
from jax import lax
from jax.experimental import pallas as pl
from jax.experimental.pallas import tpu as pltpu
from jax.sharding import PartitionSpec as P


CFG = 1024
NSETS = 512
SOFTEN = 0.04
HORIZON = 32.0
LOG2E = math.log2(math.e)
LANES = 128
SUB = 16
WIDE = 256

NT = (((1,), (1,)), ((), ()))
NN = (((1,), (0,)), ((), ()))
TN = (((0,), (0,)), ((), ()))
VM = pl.BlockSpec(memory_space=pltpu.VMEM)


def dot16(a, b, dims):
    return lax.dot_general(a, b, dims, preferred_element_type=jnp.float32)


def join(ref, blocks):
    return jnp.concatenate([ref[b] for b in blocks], axis=1)


def table_kernel(flow_ref, out_ref, date_t, high_t, one_hot, slot_a, slot_b):
    ncf, trades = flow_ref.shape[0] // 2, flow_ref.shape[1]
    blocks = trades // LANES
    row_ids = lax.broadcasted_iota(jnp.int32, (NSETS // SUB, SUB, LANES), 0) * SUB
    row_ids = (row_ids + lax.broadcasted_iota(jnp.int32, row_ids.shape, 1)).astype(jnp.int16)
    unit = jnp.ones((NSETS // SUB, SUB, LANES), jnp.bfloat16)

    def spread(row):
        return jnp.broadcast_to(row, (SUB, LANES))

    def prepare(b, carry):
        cols = pl.ds(pl.multiple_of(b * LANES, LANES), LANES)
        code = flow_ref[:ncf, cols].astype(jnp.int32)
        total = flow_ref[ncf:, cols]
        date = code & (CFG - 1)
        sets = lax.shift_right_logical(code[0:1, :], CFG.bit_length() - 1)
        for k in range(ncf):
            rows = slice(k * SUB, (k + 1) * SUB)
            date_t[b, rows, :] = spread(date[k : k + 1, :]).astype(jnp.int16)
            high_t[b, rows, :] = spread(total[k : k + 1, :]).astype(jnp.bfloat16)
        mine = spread(sets).astype(jnp.int16)[None]
        chosen = jnp.where(row_ids == mine, unit, jnp.zeros_like(unit))
        one_hot[b] = chosen.reshape(NSETS, LANES)
        return carry

    lax.fori_loop(0, blocks, prepare, 0)

    tiles = 16
    step = tiles * SUB
    parts = CFG // WIDE
    chunk = blocks // 2
    base = lax.broadcasted_iota(jnp.int32, (tiles, SUB, LANES), 0) * SUB
    base = base + lax.broadcasted_iota(jnp.int32, (tiles, SUB, LANES), 1)
    slots = (slot_a, slot_b)

    def fill(slot, part, b):
        for r in range(0, WIDE, step):
            want = (base + (part * WIDE + r)).astype(jnp.int16)
            acc = jnp.zeros((tiles, SUB, LANES), jnp.bfloat16)
            for k in range(ncf):
                rows = slice(k * SUB, (k + 1) * SUB)
                acc = jnp.where(want == date_t[b, rows, :][None], high_t[b, rows, :][None], acc)
            slot[b, r : r + step, :] = acc.reshape(step, LANES)

    def multiply(slot, part, rows):
        left = jnp.concatenate([one_hot[b, rows, :] for b in range(blocks)], axis=1)
        block = dot16(left, join(slot, range(blocks)), NT).astype(jnp.bfloat16)
        for i in range(WIDE // LANES):
            place = part * (WIDE // LANES) + i
            out_ref[place, rows, :] = block[:, i * LANES : (i + 1) * LANES]

    for part in range(parts):
        target, source = slots[part % 2], slots[(part + 1) % 2]

        def body(q, carry, part=part, target=target, source=source):
            if part > 0:
                half = pl.ds(pl.multiple_of(q * (NSETS // 2), NSETS // 2), NSETS // 2)
                multiply(source, part - 1, half)
            for i in range(chunk):
                fill(target, part, q * chunk + i)
            return carry

        lax.fori_loop(0, 2, body, 0)
    multiply(slots[(parts + 1) % 2], parts - 1, slice(0, NSETS))


def build_table(flows):
    ncf, trades = flows.shape[0] // 2, flows.shape[1]
    blocks = trades // LANES
    return pl.pallas_call(
        table_kernel,
        out_shape=jax.ShapeDtypeStruct((CFG // LANES, NSETS, LANES), jnp.bfloat16),
        in_specs=[VM],
        out_specs=VM,
        scratch_shapes=[
            pltpu.VMEM((blocks, ncf * SUB, LANES), jnp.int16),
            pltpu.VMEM((blocks, ncf * SUB, LANES), jnp.bfloat16),
            pltpu.VMEM((blocks, NSETS, LANES), jnp.bfloat16),
            pltpu.VMEM((blocks, WIDE, LANES), jnp.bfloat16),
            pltpu.VMEM((blocks, WIDE, LANES), jnp.bfloat16),
        ],
        cost_estimate=pl.CostEstimate(
            flops=4 * trades * NSETS * CFG, bytes_accessed=2**21, transcendentals=0
        ),
        compiler_params=pltpu.CompilerParams(vmem_limit_bytes=12 * 2**20),
    )(flows)


def prepare_kernel(groups, stations, scale, *refs):
    sources, outs, scratch = refs[:6], refs[6 : 11 + groups], refs[11 + groups :]
    flow_ref, left_ref, column_ref, pick_ref, route_ref, *pieces = outs
    copies = [
        pltpu.make_async_copy(source, held, scratch[6].at[i])
        for i, (source, held) in enumerate(zip(sources, scratch[:6]))
    ]
    for copy in copies:
        copy.start()
    index_ref, amount_ref, set_ref, curve_ref, weight_ref, slot_ref = scratch[:6]
    ncf = index_ref.shape[0]
    slots, nodes, total_paths = curve_ref.shape
    paths = total_paths // groups
    dates = slot_ref.shape[0]
    station, member = lax.axis_index("path"), lax.axis_index("ccy")
    copies[5].wait()
    starts, lines = [], []
    for k in range(slots):
        date, found = 0, 0
        for d in range(dates):
            hit = slot_ref[d] == station * slots + k
            date = jnp.where(hit, d, date)
            found = jnp.where(hit, 1, found)
        starts.append(0.5 * (date.astype(jnp.float32) + 1.0))
        lines.append((date, found))
    lane = lax.broadcasted_iota(jnp.int32, (CFG, slots * nodes), 1)
    start = jnp.zeros((CFG, slots * nodes), jnp.float32)
    for k in range(slots):
        start = jnp.where(lane >= k * nodes, starts[k], start)
    grid = lax.broadcasted_iota(jnp.int32, (CFG, slots * nodes), 0).astype(jnp.float32)
    remain = HORIZON * (grid + 1.0) / CFG - start
    node = (lane & (nodes - 1)).astype(jnp.float32)
    tenor = HORIZON * (node + 1.0) / nodes
    clipped = jnp.clip(remain, HORIZON / nodes, HORIZON)
    weight = jnp.maximum(0.0, 1.0 - jnp.abs(clipped - tenor) * (nodes / HORIZON))
    scaled = weight * (remain * (-LOG2E))
    high = scaled.astype(jnp.bfloat16)
    rest = scaled - high.astype(jnp.float32)
    mid = rest.astype(jnp.bfloat16)
    low = (rest - mid.astype(jnp.float32)).astype(jnp.bfloat16)
    dead = jnp.where((node == 0.0) & (remain <= 0.0), -1e30, 0.0).astype(jnp.bfloat16)
    for k in range(slots):
        own = slice(k * nodes, (k + 1) * nodes)
        left = jnp.concatenate([part[:, own] for part in (high, mid, low, dead)], axis=1)
        for i in range(4 * nodes // LANES):
            left_ref[k, i] = left[:, i * LANES : (i + 1) * LANES]
    line = lax.broadcasted_iota(jnp.int32, (dates, LANES), 0)
    slot_of = jnp.zeros((dates, LANES), jnp.int32)
    for d in range(dates):
        slot_of = jnp.where(line == d, slot_ref[d], slot_of)
    for i in range(stations * slots):
        pick_ref[i] = (slot_of == i).astype(jnp.float32)
    for g in range(groups):
        for m in range(groups):
            chosen = ((member ^ g) == m).astype(jnp.float32)
            route_ref[g * groups + m] = jnp.full((8, LANES), chosen, jnp.float32)
    for copy in copies[:5]:
        copy.wait()

    def pack(b, carry):
        cols = pl.ds(pl.multiple_of(b * LANES, LANES), LANES)
        date, amount = index_ref[:, cols], amount_ref[:, cols]
        flow_ref[:ncf, cols] = (date + CFG * set_ref[:, cols]).astype(jnp.float32)
        total = jnp.zeros((ncf, LANES), jnp.float32)
        for k in range(ncf):
            same = date == date[k : k + 1, :]
            total = total + jnp.where(same, amount[k : k + 1, :], 0.0)
        flow_ref[ncf:, cols] = total
        return carry

    lax.fori_loop(0, index_ref.shape[1] // LANES, pack, 0)
    for mask, piece in enumerate(pieces):
        begin = pl.multiple_of((member ^ mask) * paths, LANES)
        for k in range(slots):
            piece[k] = curve_ref[k, :, pl.ds(begin, paths)]
    term = lax.broadcasted_iota(jnp.int32, (SUB, NSETS), 0)
    for k, (date, found) in enumerate(lines):
        row = weight_ref[pl.ds(date, 1), :] * (0.5 * scale) * found.astype(jnp.float32)
        rest = jnp.broadcast_to(row, (SUB, NSETS))
        terms = jnp.zeros((SUB, NSETS), jnp.float32)
        for i in range(3):
            part = rest.astype(jnp.bfloat16).astype(jnp.float32)
            terms = jnp.where(term == i, part, terms)
            rest = rest - part
        column_ref[k] = dot16(
            terms.astype(jnp.bfloat16), jnp.ones((SUB, LANES), jnp.bfloat16), TN
        )


def prepare(date_slot, index, amount, sets, curve, weights, groups, stations):
    ncf, trades = index.shape
    slots, nodes, total_paths = curve.shape
    dates = date_slot.shape[0]
    sources = (index, amount, sets, curve, weights, date_slot)
    return pl.pallas_call(
        functools.partial(prepare_kernel, groups, stations, 1.0 / total_paths),
        out_shape=(
            jax.ShapeDtypeStruct((2 * ncf, trades), jnp.float32),
            jax.ShapeDtypeStruct((slots, 4 * nodes // LANES, CFG, LANES), jnp.bfloat16),
            jax.ShapeDtypeStruct((slots, NSETS, LANES), jnp.float32),
            jax.ShapeDtypeStruct((stations * slots, dates, LANES), jnp.float32),
            jax.ShapeDtypeStruct((groups * groups, 8, LANES), jnp.float32),
        )
        + (jax.ShapeDtypeStruct((slots, nodes, total_paths // groups), jnp.bfloat16),) * groups,
        in_specs=[pl.BlockSpec(memory_space=pltpu.HBM)] * 6,
        out_specs=(VM,) * (5 + groups),
        scratch_shapes=[pltpu.VMEM(source.shape, source.dtype) for source in sources[:5]]
        + [pltpu.SMEM((dates,), jnp.int32), pltpu.SemaphoreType.DMA((6,))],
        cost_estimate=pl.CostEstimate(flops=2**22, bytes_accessed=2**21, transcendentals=0),
        compiler_params=pltpu.CompilerParams(
            vmem_limit_bytes=14 * 2**20 + 6 * slots * nodes * total_paths
        ),
        name="prepare",
    )(*[pltpu.with_memory_space_constraint(source, pltpu.HBM) for source in sources])


def grant(own, shared):
    return own if shared <= 2**24 else 62 * 2**20


def disc_kernel(groups, left_ref, *refs):
    curves, (disc_ref, rhs) = refs[:groups], refs[groups:]
    slots, nodes, paths = curves[0].shape
    depth = rhs.shape[0]
    rhs[3 * nodes :, :] = jnp.ones((depth - 3 * nodes, paths), jnp.bfloat16)
    for k in range(slots):
        left = join(left_ref.at[k], range(depth // LANES))
        for g in range(groups):
            for copy in range(3):
                rhs[copy * nodes : (copy + 1) * nodes, :] = curves[g][k]
            for p0 in range(0, paths, WIDE):
                block = jnp.exp2(dot16(left, rhs[:, p0 : p0 + WIDE], NN)).astype(jnp.bfloat16)
                for i in range(WIDE // LANES):
                    disc_ref[k, g, p0 // LANES + i] = block[:, i * LANES : (i + 1) * LANES]


def discounts(left, curves):
    slots, nodes, paths = curves[0].shape
    groups = len(curves)
    return pl.pallas_call(
        functools.partial(disc_kernel, groups),
        out_shape=jax.ShapeDtypeStruct(
            (slots, groups, paths // LANES, CFG, LANES), jnp.bfloat16
        ),
        in_specs=[VM] * (1 + groups),
        out_specs=VM,
        scratch_shapes=[pltpu.VMEM((4 * nodes, paths), jnp.bfloat16)],
        cost_estimate=pl.CostEstimate(
            flops=2 * slots * groups * CFG * paths * 4 * nodes,
            bytes_accessed=2 * slots * groups * CFG * paths,
            transcendentals=slots * groups * CFG * paths,
        ),
        compiler_params=pltpu.CompilerParams(
            vmem_limit_bytes=grant(6 * 2**20, 2 * slots * groups * CFG * paths)
        ),
        name="discounts",
    )(left, *curves)


def price_kernel(stations, scale, column_ref, left_ref, route_ref, disc_ref, *refs):
    groups = disc_ref.shape[1]
    tables = refs[:groups]
    out_ref, value_ref, slope_ref, expo_ref, pull_ref, sens_ref = refs[groups:]
    slots = disc_ref.shape[0]
    pblocks = disc_ref.shape[2]
    cblocks = CFG // LANES
    nodes = sens_ref.shape[2]
    share = NSETS // groups
    wide = WIDE // LANES
    pull_ref[...] = jnp.zeros_like(pull_ref)

    def values(k, p0):
        left = jnp.concatenate([join(tables[g], range(cblocks)) for g in range(groups)], axis=1)
        right = jnp.concatenate(
            [join(disc_ref.at[k, g], range(p0, p0 + wide)) for g in range(groups)], axis=0
        )
        value = dot16(left, right, NN)
        for i in range(wide):
            value_ref[k, p0 + i] = value[:, i * LANES : (i + 1) * LANES]

    def slopes(k):
        column = column_ref[k]
        folded = jnp.zeros((NSETS, LANES), jnp.float32)
        for p in range(pblocks):
            part = value_ref[k, p]
            square = part * part + SOFTEN
            inverse = lax.rsqrt(square)
            folded = folded + (part + square * inverse)
            slope = column + column * (part * inverse)
            slope_ref[k, p] = slope.astype(jnp.bfloat16)
        summed = jnp.zeros((SUB, NSETS), jnp.float32)
        for _ in range(3):
            term = folded.astype(jnp.bfloat16)
            folded = folded - term.astype(jnp.float32)
            summed = summed + dot16(jnp.ones((SUB, LANES), jnp.bfloat16), term, NT)
        expo_ref[k : k + 1, :] = summed[0:1] * (0.5 * scale)

    def pulls(k, g):
        slope_all = join(slope_ref.at[k], range(pblocks))
        for c0 in range(0, cblocks, wide):
            right = jnp.concatenate(
                [disc_ref[k, g, p, c0 * LANES : (c0 + wide) * LANES, :] for p in range(pblocks)],
                axis=1,
            )
            back = dot16(slope_all, right, NT)
            for i in range(wide):
                cash = tables[g][c0 + i].astype(jnp.float32)
                pull = jnp.sum(back[:, i * LANES : (i + 1) * LANES] * cash, axis=0)
                cols = slice((c0 + i) * LANES, (c0 + i + 1) * LANES)
                pull_ref[k, g : g + 1, cols] = pull[None]

    for p0 in range(0, pblocks, wide):
        values(0, p0)
    for k in range(slots):
        beside = []
        if k + 1 < slots:
            beside = [functools.partial(values, k + 1, p0) for p0 in range(0, pblocks, wide)]
        elif k > 0:
            beside = [functools.partial(pulls, k - 1, g) for g in range(groups)]
        for work in beside[:1]:
            work()
        slopes(k)
        for work in beside[1:]:
            work()
    for k in [*range(slots - 2), slots - 1]:
        for g in range(groups):
            pulls(k, g)
    for k in range(slots):
        pull = pull_ref[k]
        terms = []
        for _ in range(3):
            term = pull.astype(jnp.bfloat16)
            pull = pull - term.astype(jnp.float32)
            terms.append(term.astype(jnp.float32))
        rows = jnp.concatenate(terms, axis=0).astype(jnp.bfloat16)
        crossed = dot16(rows, join(left_ref.at[k], range(left_ref.shape[1])), NN)
        count = pull_ref.shape[1]
        sens = jnp.zeros((count, nodes), jnp.float32)
        for i in range(3):
            for j in range(3):
                sens = sens + crossed[i * count : (i + 1) * count, j * nodes : (j + 1) * nodes]
        sens_ref[k] = sens * (1.0 / LOG2E)
    for g in range(groups):
        rows = slice(g * stations, (g + 1) * stations)
        for k in range(slots):
            part = expo_ref[k : k + 1, g * share : (g + 1) * share]
            out_ref[rows, 0, k * share : (k + 1) * share] = jnp.broadcast_to(
                part, (stations, share)
            )
            line = jnp.zeros((1, nodes), jnp.float32)
            for m in range(groups):
                line = line + route_ref[g * groups + m, 0:1, :nodes] * sens_ref[k, m : m + 1, :]
            begin = slots * share + k * nodes
            out_ref[rows, 0, begin : begin + nodes] = jnp.broadcast_to(line, (stations, nodes))


def price(column, left, route, disc, tables, stations, total_paths):
    slots, groups, pblocks = disc.shape[:3]
    nodes = left.shape[1] * LANES // 4
    paths = pblocks * LANES
    rows = -(-groups // 8) * 8
    return pl.pallas_call(
        functools.partial(price_kernel, stations, 1.0 / total_paths),
        out_shape=jax.ShapeDtypeStruct(
            (groups * stations, 1, slots * (NSETS // groups + nodes)), jnp.float32
        ),
        in_specs=[VM] * (4 + groups),
        out_specs=VM,
        scratch_shapes=[
            pltpu.VMEM((slots, pblocks, NSETS, LANES), jnp.float32),
            pltpu.VMEM((slots, pblocks, NSETS, LANES), jnp.bfloat16),
            pltpu.VMEM((slots, NSETS), jnp.float32),
            pltpu.VMEM((slots, rows, CFG), jnp.float32),
            pltpu.VMEM((slots, rows, nodes), jnp.float32),
        ],
        cost_estimate=pl.CostEstimate(
            flops=4 * slots * groups * CFG * paths * NSETS,
            bytes_accessed=2 * slots * groups * CFG * paths,
            transcendentals=slots * NSETS * paths,
        ),
        compiler_params=pltpu.CompilerParams(
            vmem_limit_bytes=grant(10 * 2**20, 2 * slots * groups * CFG * paths)
        ),
        name="price",
    )(column, left, route, disc, *tables)


def collect_kernel(groups, slots, nodes, pick_ref, got_ref, expo_ref, sens_ref):
    stations = got_ref.shape[0] // groups
    dates, share = expo_ref.shape
    expo = jnp.zeros((dates, share), jnp.float32)
    sens = jnp.zeros((dates, nodes), jnp.float32)
    for p in range(stations):
        line = got_ref[p]
        for g in range(1, groups):
            line = line + got_ref[g * stations + p]
        for k in range(slots):
            pick = pick_ref[p * slots + k]
            begin = slots * share + k * nodes
            mine = pick[:, :share] if share <= LANES else pick[:, :1]
            expo = expo + mine * line[:, k * share : (k + 1) * share]
            sens = sens + pick[:, :nodes] * line[:, begin : begin + nodes]
    expo_ref[...] = expo
    sens_ref[...] = sens


def collect(pick, got, groups, slots, nodes):
    dates = pick.shape[1]
    return pl.pallas_call(
        functools.partial(collect_kernel, groups, slots, nodes),
        out_shape=(
            jax.ShapeDtypeStruct((dates, NSETS // groups), jnp.float32),
            jax.ShapeDtypeStruct((dates, nodes), jnp.float32),
        ),
        in_specs=[VM, VM],
        out_specs=(VM, VM),
        compiler_params=pltpu.CompilerParams(vmem_limit_bytes=6 * 2**20),
        name="collect",
    )(pick, got)


def local(curve_store, cash_index, cash_amount, trade_set, date_slot, default_weight):
    groups = lax.axis_size("ccy")
    stations = lax.axis_size("path")
    _, slots, nodes, total_paths = curve_store.shape

    def swap(array, mask):
        return lax.ppermute(array, "ccy", [(i, i ^ mask) for i in range(groups)])

    flows, left, column, pick, route, *pieces = prepare(
        date_slot, jnp.swapaxes(cash_index[0], 0, 1), jnp.swapaxes(cash_amount[0], 0, 1),
        trade_set, curve_store[0], default_weight, groups, stations,
    )
    others = {m: swap(flows, m) for m in range(2, groups, 2)}
    curves = [pieces[0]] + [swap(pieces[m], m) for m in range(1, groups)]

    tables = {0: build_table(flows)}
    for m in others:
        tables[m] = build_table(others[m])
    for m in list(tables):
        tables[m + 1] = swap(tables[m], 1)
    tables = [tables[m] for m in range(groups)]

    disc = discounts(left, curves)
    payload = price(column, left, route, disc, tables, stations, total_paths)
    got = lax.all_to_all(payload, ("ccy", "path"), 0, 0, tiled=True)
    expo, sens = collect(pick, got, groups, slots, nodes)
    return expo, sens[None]


def solution(mesh):
    in_specs = (
        P("ccy", "path", None, None),
        P("ccy", None, None),
        P("ccy", None, None),
        P("ccy", None),
        P(),
        P(),
    )
    out_specs = (P(None, "ccy"), P("ccy", None, None))
    return jax.shard_map(local, mesh=mesh, in_specs=in_specs, out_specs=out_specs, check_vma=False)
```
